256 devices in a mesh: row: 16 (over x, y_hi, core), col: 16 (over y_lo, z).
Axes of the slice: x: 4, y: 4 (y_hi: 2, y_lo: 2; y = y_hi * 2 + y_lo), z: 8, core: 2. Of those that a mesh axis runs over, the one named last changes fastest.
Arguments:
- expression: bfloat16 [32768, 1024], P(('row', 'col')), may hold values from -200 to 200, as said below
- powers: int32 [10], replicated, may hold values from 1 to 20
Outputs:
- log_degree: float32 [10, 32768], P(None, ('row', 'col'))
- degree_freq: float32 [10, 10], replicated
- fit_slope: float32 [10], replicated
- mean_log: float32 [10], replicated
The draws below stay inside these ranges and needn't reach their ends.
Inputs may be any that keep to these rules, and one draw needn't show every extreme that they name: Finite expression values.
All inputs are finite; a program needn't handle non-finite values.
Results may differ from the reference program's by a relative error of at most 0.0003.
Values may be sent and summed in bfloat16 or wider, within the bound.
A program may use at most 64 MiB of HBM per device.

```python
import math
import jax
import jax.numpy as jnp
from jax import lax

S = 1024
NPOW = 10
BINS = 10
MODULES = 400
GENES = 32768


def draw_expression(key, part):
    keys = jax.random.split(key, 10)
    leading_count = max(MODULES // 8, 1)
    leading_ids = jax.random.randint(keys[0], (GENES, 1), 0, leading_count)
    other_ids = jax.random.randint(keys[8], (GENES, 7), 0, MODULES)
    factor_ids = jnp.concatenate([leading_ids, other_ids], axis=1)
    live_count = jax.random.randint(keys[1], (GENES, 1), 1, 6)
    slot_index = jnp.arange(8, dtype=jnp.int32)[None, :]
    leading_strength = jax.random.uniform(keys[2], (GENES, 1), jnp.float32, 0.85, 1.0)
    other_strength = jax.random.uniform(keys[9], (GENES, 7), jnp.float32, 0.1, 0.3)
    strength = jnp.concatenate([leading_strength, other_strength], axis=1)
    signs = (jax.random.randint(keys[3], (GENES, 8), 0, 2) * 2 - 1).astype(jnp.float32)
    loading = jnp.where(slot_index < live_count, strength * signs, 0.0)
    factors = jax.random.normal(keys[4], (MODULES, S), jnp.float32)
    signal = jnp.zeros((GENES, S), jnp.float32)
    for slot in range(8):
        signal = signal + loading[:, slot:slot + 1] * jnp.take(factors, factor_ids[:, slot], axis=0)
    noise_scale = jnp.exp(jax.random.uniform(keys[5], (GENES, 1), jnp.float32, -3.0, 1.0))
    noise_part = jax.random.normal(keys[6], (GENES, S), jnp.float32)
    total = jnp.sum(loading * loading, axis=1, keepdims=True) + noise_scale * noise_scale
    values = (signal + noise_scale * noise_part) / jnp.sqrt(total)
    return values.astype(jnp.bfloat16)


def place_ends(result, own_key, least, top_value):
    shape = result.shape
    spot = [jax.random.randint(jax.random.fold_in(own_key, axis), (), 0, shape[axis]) for axis in range(len(shape))]
    result = result.at[tuple(spot)].set(least)
    longest = shape.index(max(shape))
    spot[longest] = (spot[longest] + 1) % shape[longest]
    return result.at[tuple(spot)].set(top_value)


def setup_inputs(seed: int = 0) -> dict:
    arg_keys = jax.random.split(jax.random.key(seed), 3)
    expression = draw_expression(jax.random.fold_in(arg_keys[2], 71), 0)
    powers = place_ends(jax.random.randint(arg_keys[1], (NPOW,), 1, 21), jax.random.fold_in(arg_keys[1], 1), 1, 20).astype(jnp.int32)
    return dict(expression=expression, powers=powers)


def reference(expression, powers):
    values = expression.astype(jnp.float32)
    gene_mean = lax.optimization_barrier(jnp.mean(values, axis=1))
    centred = values - gene_mean[:, None]
    gene_inv = lax.rsqrt(lax.optimization_barrier(jnp.mean(centred * centred, axis=1)) + 1e-06)
    exponents = powers.astype(jnp.float32)
    block_rows = math.gcd(GENES, 512)
    blocks = GENES // block_rows

    def one_block(packed):
        row_block, block_mean, block_inv = packed
        raw = jnp.dot(row_block, expression.T, preferred_element_type=jnp.float32)
        pearson = (raw / S - block_mean[:, None] * gene_mean[None, :]) * block_inv[:, None] * gene_inv[None, :]
        log_abs = jnp.log(jnp.abs(pearson))
        return jnp.stack([lax.optimization_barrier(jnp.sum(jnp.exp(exponents[power_index] * log_abs), axis=1)) for power_index in range(NPOW)])
    blocked = lax.map(one_block, (expression.reshape(blocks, block_rows, S), gene_mean.reshape(blocks, block_rows), gene_inv.reshape(blocks, block_rows)))
    degree = jnp.transpose(blocked, (1, 0, 2)).reshape(NPOW, GENES)
    peak = lax.optimization_barrier(jnp.max(degree, axis=1))
    position = jnp.clip(BINS * degree / peak[:, None] - 0.5, 0.0, BINS - 1.0)
    centres = jnp.arange(BINS, dtype=jnp.float32)
    weights = jnp.maximum(0.0, 1.0 - jnp.abs(position[:, :, None] - centres[None, None, :]))
    degree_freq = lax.optimization_barrier(jnp.sum(weights, axis=1)) / GENES
    mean_log = jnp.log10(lax.optimization_barrier(jnp.sum(degree, axis=1)) / GENES)
    xfit = jnp.log10((centres[None, :] + 0.5) * peak[:, None] / BINS)
    yfit = jnp.log10(degree_freq + 1.0 / GENES)
    xdev = xfit - lax.optimization_barrier(jnp.mean(xfit, axis=1, keepdims=True))
    ydev = yfit - lax.optimization_barrier(jnp.mean(yfit, axis=1, keepdims=True))
    fit_slope = lax.optimization_barrier(jnp.sum(xdev * ydev, axis=1)) / lax.optimization_barrier(jnp.sum(xdev * xdev, axis=1))
    return (jnp.log10(degree), degree_freq, fit_slope, mean_log)
```

```python
import functools
import math

import jax
import jax.numpy as jnp
from jax import lax
from jax.experimental import pallas as pl
from jax.experimental.pallas import tpu as pltpu
from jax.sharding import Mesh
from jax.sharding import PartitionSpec as P

F32 = jnp.float32
AXES = ("x", "yh", "core", "yl", "z")
NP = 10
BINS = 10
GENES = 32768
S = 1024
G = 128
MESH_ID = pl.DeviceIdType.MESH
OFFSETS = (
    0, 16, 1, 4, 112, 3, 116, 2, 124, 7, 32, 120, 96, 33, 35, 108, 11, 104, 34,
)
HOPS = (
    (0, 0, 0, 2), (0, 1, 1, 5), (0, 1, 4, 1), (0, 0, 5, 4), (0, 1, 2, 3), (0, 1, 5, 4), (0, 1, 0, 2), (0, 0,
    2, 3), (0, 0, 1, 5), (0, 0, 4, 1), (4, 0, 3, 8), (4, 0, 2, 6), (5, 1, 1, 7), (3, 1, 5, 6), (1, 1, 4, 10),
    (2, 0, 0, 7), (4, 1, 3, 8), (4, 1, 5, 12), (1, 0, 4, 10), (3, 0, 1, 9), (5, 1, 2, 9), (10, 1, 0, 13), (8,
    0, 3, 11), (10, 1, 1, 14), (4, 0, 5, 12), (6, 1, 2, 11), (10, 0, 0, 13), (12, 1, 3, 15), (9, 0, 2, 16),
    (10, 0, 1, 14), (8, 0, 5, 15), (13, 1, 0, 18), (9, 1, 2, 16), (11, 0, 5, 17), (15, 1, 3, 17), (13, 0, 0,
    18),
)
ARRIVALS = (
    (1, 1), (2, 0), (3, 1), (4, 0), (5, 1), (1, 0), (2, 1), (3, 0), (4, 1), (5, 0), (8, 0), (6, 0), (6, 1),
    (7, 0), (7, 1), (10, 1), (8, 1), (9, 0), (9, 1), (10, 0), (12, 1), (11, 0), (13, 1), (11, 1), (12, 0),
    (14, 1), (13, 0), (15, 1), (14, 0), (15, 0), (16, 0), (18, 1), (16, 1), (17, 0), (17, 1), (18, 0),
)
STEPS = ((1, 0, 0), (-1, 0, 0), (0, 1, 0), (0, -1, 0), (0, 0, 1), (0, 0, -1))
NS = len(OFFSETS)
PIECES = 2
ROWS = G // PIECES


def offset_of(e):
    return (e & 3, (e >> 2) & 3, e >> 4)


def minus(a, b):
    (ax, ay, az), (bx, by, bz) = offset_of(a), offset_of(b)
    return ((ax - bx) & 3) | (((ay - by) & 3) << 2) | (((az - bz) & 7) << 4)


def pair_plan():
    where = {e: i for i, e in enumerate(OFFSETS)}
    full, half = ({}, [])
    for d in range(1, 128):
        if minus(0, d) < d:
            continue
        found = []
        for i, e in enumerate(OFFSETS):
            j = where.get(minus(e, d))
            if j is not None:
                found.append((max(i, j), min(i, j)))
        later, earlier = min(found)
        if minus(0, d) == d:
            half.append((later, earlier, d))
        else:
            full.setdefault(later, []).append(earlier)
    return ({k: sorted(v) for k, v in full.items()}, half)


FULL, HALF = pair_plan()
LEFTS = sorted({0} | {a for v in FULL.values() for a in v} | {a for _, a, _ in HALF})
YROWS = max(max(v) - min(v) + 1 for v in [*FULL.values(), [0]])


def dot_t(a, b):
    return lax.dot_general(a, b, (((1,), (1,)), ((), ())), preferred_element_type=F32)


def coded(values, width):
    code = 0
    for v in reversed(values):
        code = code * width + v
    return code


def over_list(values, body):
    for k in range(0, len(values), 6):
        some = values[k : k + 6]

        def step(_, code):
            body(lax.rem(code, 32))
            return lax.div(code, 32)

        lax.fori_loop(0, len(some), step, jnp.int32(coded(some, 32)))


def powers_of(y, lefts, rights, exponents, rows_acc, cols_acc, halves):
    left_sum, left_inv = lefts
    mean = [jnp.broadcast_to(r[2:3, :], (8, 128)) for r in rights]
    inv = [jnp.broadcast_to(r[3:4, :], (8, 128)) for r in rights]
    cols = [[None] * halves for _ in range(NP)]
    for band in range(G // 8):
        rows = slice(8 * band, 8 * band + 8)
        m, i = (left_sum[rows, :], left_inv[rows, :])
        logs = [jnp.log2(jnp.abs((y(rows, h) - m * mean[h]) * i * inv[h])) for h in range(halves)]
        for p in range(NP):
            total = None
            for h in range(halves):
                q = jnp.exp2(exponents[p] * logs[h])
                cols[p][h] = q if cols[p][h] is None else cols[p][h] + q
                total = q if total is None else total + q
            rows_acc[p, rows, :] = rows_acc[p, rows, :] + total
    for p in range(NP):
        for h in range(halves):
            cols_acc(h, p, cols[p][h])


def lane_row(column):
    return jnp.broadcast_to(column, (128, 128)).T[0:8, :]


def kernel(
    pw, e, logdeg_out, freq_out, small_out,
    X, Y, YI, racc, cacc, LM, LI, ST, PS, RB, DG, ZA, ZB, tile, dsrc, fsrc,
    piece_send, piece_recv, pair_send, pair_recv, stat_send, stat_recv,
    part_send, part_recv, plane_send, plane_recv, za_send, za_recv, zb_send, zb_recv,
):
    px, pyh, c, pyl, pz = [lax.axis_index(a) for a in AXES]
    py = pyh * 2 + pyl
    other = 1 - c

    def at(dx, dy, dz, core):
        y = lax.rem(py + dy + 8, 4)
        return (lax.rem(px + dx + 8, 4), lax.div(y, 2), core, lax.rem(y, 2), lax.rem(pz + dz + 16, 8))

    def remote(src, dst, send, recv, device):
        return pltpu.make_async_remote_copy(
            src_ref=src, dst_ref=dst, send_sem=send, recv_sem=recv, device_id=device, device_id_type=MESH_ID
        )

    partner = at(0, 0, 0, other)
    exponents = [pw[p].astype(F32) for p in range(NP)]

    def piece(slot, q, half):
        return X.at[half, slot, ROWS * q : ROWS * q + ROWS, :]

    def own(q):
        return e.at[ROWS * q : ROWS * q + ROWS, :]

    def hop(i, q, k, j):
        dx, dy, dz = STEPS[k]
        src = own(q) if i == 0 else piece(i, q, c)
        return remote(src, piece(j, q, c), piece_send, piece_recv.at[j * PIECES + q], at(-dx, -dy, -dz, c))

    def to_partner(slot, q):
        src = own(q) if slot == 0 else piece(slot, q, c)
        return remote(src, piece(slot, q, c), pair_send, pair_recv.at[slot * PIECES + q], partner)

    for i, q, k, j in HOPS:
        if i == 0:
            hop(i, q, k, j).start()
    for q in range(PIECES):
        to_partner(0, q).start()

    X[c, 0, :, :] = e[...]
    values = e[...].astype(F32)
    total = jnp.sum(values, axis=1, keepdims=True)
    gene_mean = total * (1.0 / S)
    centred = values - gene_mean
    gene_inv = lax.rsqrt(jnp.sum(centred * centred, axis=1, keepdims=True) * (1.0 / S) + 1e-06)
    row_id = lax.broadcasted_iota(jnp.int32, (8, 128), 0)
    sum_row, inv_row = (lane_row(total), lane_row(gene_inv))
    stats = jnp.where(row_id == 0, sum_row, jnp.where(row_id == 1, inv_row, jnp.where(row_id == 2, sum_row * (1.0 / S), inv_row * (1.0 / S))))
    tile[...] = stats
    ST[pl.ds(c, 1)] = stats[None]

    def stat(slot, half):
        x, y, z = offset_of(OFFSETS[slot])
        return remote(tile, ST.at[2 * slot + c], stat_send, stat_recv.at[2 * slot + c], at(-x, -y, -z, half))

    def stat_in(slot, half):
        x, y, z = offset_of(OFFSETS[slot])
        return remote(tile, ST.at[2 * slot + half], stat_send, stat_recv.at[2 * slot + half], at(-x, -y, -z, half))

    stat(0, other).start()
    for slot in range(1, NS):
        for half in range(2):
            stat(slot, half).start()

    zero = jnp.zeros((NP, 8, 128), F32)

    def clear_rows(s, _):
        for b in range(G // 8):
            racc[s, :, 8 * b : 8 * b + 8, :] = zero
        return 0

    def clear_cols(s, _):
        cacc[s, 0] = zero
        cacc[s, 1] = zero
        return 0

    lax.fori_loop(0, NS, clear_rows, 0)
    lax.fori_loop(0, NS + 1, clear_cols, 0)
    for h in range(2):
        PS[:, h, :, :] = jnp.zeros((NS, 16, 128), F32)

    def ready(slot):
        for q in range(PIECES):
            remote(piece(slot, q, other), piece(slot, q, other), pair_send, pair_recv.at[slot * PIECES + q], partner).wait_recv()
        if slot == 0:
            stat_in(0, other).wait_recv()
        else:
            for half in range(2):
                stat_in(slot, half).wait_recv()
        if slot in LEFTS:
            mine = ST[2 * slot + c]
            LM[slot] = jnp.broadcast_to(mine[0:1, :], (128, 128)).T
            LI[slot] = jnp.broadcast_to(mine[1:2, :], (128, 128)).T

    def block(a, y_row, b, cols_slot):
        y_at = pl.multiple_of(y_row * G, G)

        def y(rows, h):
            return Y[pl.ds(y_at + rows.start, 8), 128 * h : 128 * h + 128]

        def add(h, p, v):
            cacc[cols_slot, h, p] = cacc[cols_slot, h, p] + v

        powers_of(y, (LM.at[a], LI.at[a]), [ST[2 * b], ST[2 * b + 1]], exponents, racc.at[a], add, 2)

    def rhs_of(b):
        return X[:, b].reshape(2 * G, S)

    ready(0)
    Y[0:G, :] = dot_t(X[c, 0], rhs_of(0))
    lax.fori_loop(0, 1, lambda _, x: (block(0, 0, 0, NS), x)[1], 0)

    seen = {s: 0 for s in range(1, NS)}
    for slot, q in ARRIVALS:
        remote(piece(slot, q, c), piece(slot, q, c), piece_send, piece_recv.at[slot * PIECES + q], partner).wait_recv()
        for h in HOPS:
            if h[0] == slot and h[1] == q:
                hop(*h).start()
        to_partner(slot, q).start()
        seen[slot] += 1
        if seen[slot] < PIECES:
            continue
        ready(slot)
        lefts = FULL.get(slot, [])
        if lefts:
            lo, hi = (min(lefts), max(lefts) + 1)
            Y[0 : (hi - lo) * G, :] = dot_t(X[c, lo:hi].reshape((hi - lo) * G, S), rhs_of(slot))
            over_list(lefts, lambda a, lo=lo, slot=slot: block(a, a - lo, slot, slot))
        for n, (b, a, _) in enumerate(HALF):
            if b == slot:
                YI[n] = dot_t(X[c, a], rhs_of(b))

    def half_block(n, d, a, b):
        x, y, z = offset_of(d)
        turn = lax.rem(lax.div(px, 2), 2) if x else lax.rem(lax.div(py, 2), 2) if y else lax.rem(lax.div(pz, 4), 2)
        h = lax.rem(c + turn, 2)

        def add(_, p, v):
            cacc[b, h, p] = cacc[b, h, p] + v

        lanes = pl.ds(pl.multiple_of(h * 128, 128), 128)
        powers_of(lambda rows, _: YI[n, rows, lanes], (LM.at[a], LI.at[a]), [ST[2 * b + h]], exponents, racc.at[a], add, 1)

    for n, (b, a, d) in enumerate(HALF):
        half_block(n, d, a, b)

    lane_id = lax.broadcasted_iota(jnp.int32, (128, 128), 1)

    def gather_cols(s, _):
        for h in range(2):
            PS[s, h, 0:NP, :] = jnp.sum(cacc[s, h], axis=1)
        return 0

    def gather_rows(s):
        sums = jnp.zeros((128, 128), F32)
        for p in range(NP):
            sums = jnp.where(lane_id == p, jnp.sum(racc[s, p], axis=1, keepdims=True), sums)
        PS[s, c, 0:NP, :] = PS[s, c, 0:NP, :] + sums.T[0:NP, :]

    lax.fori_loop(1, NS, gather_cols, 0)
    over_list(LEFTS, gather_rows)

    def part(slot, half):
        x, y, z = offset_of(OFFSETS[slot])
        return remote(PS.at[slot, half], RB.at[2 * slot + c], part_send, part_recv.at[2 * slot + c], at(x, y, z, half))

    for slot in range(1, NS):
        for half in range(2):
            part(slot, half).start()
    degree = PS[0, c]
    for slot in range(1, NS):
        for half in range(2):
            remote(PS.at[slot, half], RB.at[2 * slot + half], part_send, part_recv.at[2 * slot + half], partner).wait_recv()
    degree = lax.fori_loop(2, 2 * NS, lambda k, d: d + RB[k], degree)
    dsrc[...] = degree

    me = (px * 4 + py) * 2 + c
    DG[pl.ds(me, 1)] = degree[None]
    plane = [(dx, dy, dc) for dx in range(4) for dy in range(4) for dc in range(2) if (dx, dy, dc) != (0, 0, 0)]

    def plane_hop(n, dx, dy, dc):
        return remote(dsrc, DG.at[me], plane_send, plane_recv.at[n], at(dx, dy, 0, lax.rem(c + dc, 2)))

    def plane_in(n, dx, dy, dc):
        x, yh, core, yl, _ = at(-dx, -dy, 0, lax.rem(c + dc, 2))
        k = (x * 4 + yh * 2 + yl) * 2 + core
        return remote(dsrc, DG.at[k], plane_send, plane_recv.at[n], partner)

    for n, h in enumerate(plane):
        plane_hop(n, *h).start()
    logdeg_out[...] = (jnp.log(degree) * (1.0 / math.log(10.0)))[0:NP, :]
    for n, h in enumerate(plane):
        plane_in(n, *h).wait_recv()

    def most(k, m):
        return jnp.maximum(m, DG[k])

    top = jnp.broadcast_to(jnp.max(lax.fori_loop(1, 32, most, DG[0]), axis=1, keepdims=True), (16, 128))

    def ring(src, buf, send, recv):
        buf[pl.ds(pz, 1)] = src[...][None]
        for dz in range(1, 8):
            remote(src, buf.at[pz], send, recv.at[dz], at(0, 0, dz, c)).start()
        for dz in range(1, 8):
            remote(src, buf.at[lax.rem(pz - dz + 8, 8)], send, recv.at[dz], partner).wait_recv()

    dsrc2 = fsrc.at[0]
    dsrc2[...] = top
    ring(dsrc2, ZA, za_send, za_recv)
    peak = functools.reduce(jnp.maximum, [ZA[k] for k in range(8)])

    def weights(k, sums):
        d = DG[k]
        position = jnp.clip(BINS * d / peak - 0.5, 0.0, BINS - 1.0)
        near = [jnp.maximum(0.0, 1.0 - jnp.abs(position - float(b))) for b in range(BINS)]
        return tuple(s + v for s, v in zip(sums, [*near, d], strict=True))

    sums = lax.fori_loop(0, 32, weights, tuple(jnp.zeros((16, 128), F32) for _ in range(BINS + 1)))
    lanes = lax.broadcasted_iota(jnp.int32, (16, 128), 1)
    found = jnp.zeros((16, 128), F32)
    for b in range(BINS + 1):
        found = jnp.where(lanes == b, jnp.sum(sums[b], axis=1, keepdims=True), found)
    fsrc[1] = found
    ring(fsrc.at[1], ZB, zb_send, zb_recv)
    totals = functools.reduce(lambda u, v: u + v, [ZB[k] for k in range(8)])

    log10 = 1.0 / math.log(10.0)
    used = lanes < BINS
    freq = totals * (1.0 / GENES)
    fit_x = jnp.where(used, jnp.log((lanes.astype(F32) + 0.5) * peak / BINS) * log10, 0.0)
    fit_y = jnp.where(used, jnp.log(freq + 1.0 / GENES) * log10, 0.0)
    dev_x = jnp.where(used, fit_x - jnp.sum(fit_x, axis=1, keepdims=True) / BINS, 0.0)
    dev_y = jnp.where(used, fit_y - jnp.sum(fit_y, axis=1, keepdims=True) / BINS, 0.0)
    slope = jnp.sum(dev_x * dev_y, axis=1, keepdims=True) / jnp.sum(dev_x * dev_x, axis=1, keepdims=True)
    mean_log = jnp.log(freq[:, BINS : BINS + 1]) * log10
    freq_out[...] = freq[0:NP, 0:BINS]
    small_out[...] = jnp.where(lanes == 0, slope, mean_log)[0:NP, :]

    half_x = X.at[0]
    pltpu.make_async_copy(half_x.at[0 : NS - 1], half_x.at[0 : NS - 1], piece_send).wait()
    pltpu.make_async_copy(half_x, half_x, pair_send).wait()
    pltpu.make_async_copy(ST.at[0 : 2 * NS - 1], ST.at[0 : 2 * NS - 1], stat_send).wait()
    pltpu.make_async_copy(RB.at[0 : 2 * NS - 2], RB.at[0 : 2 * NS - 2], part_send).wait()
    pltpu.make_async_copy(DG.at[0:31], DG.at[0:31], plane_send).wait()
    pltpu.make_async_copy(ZA.at[0:7], ZA.at[0:7], za_send).wait()
    pltpu.make_async_copy(ZB.at[0:7], ZB.at[0:7], zb_send).wait()


def on_device(expression, powers):
    dma = pltpu.SemaphoreType.DMA
    vmem = pl.BlockSpec(memory_space=pltpu.VMEM)
    logdeg, freq, small = pl.pallas_call(
        kernel,
        out_shape=[
            jax.ShapeDtypeStruct((NP, G), F32),
            jax.ShapeDtypeStruct((NP, BINS), F32),
            jax.ShapeDtypeStruct((NP, 128), F32),
        ],
        in_specs=[pl.BlockSpec(memory_space=pltpu.SMEM), vmem],
        out_specs=[vmem] * 3,
        scratch_shapes=[
            pltpu.VMEM((2, NS, G, S), jnp.bfloat16),
            pltpu.VMEM((YROWS * G, 2 * G), F32),
            pltpu.VMEM((len(HALF), G, 2 * G), F32),
            pltpu.VMEM((NS, NP, G, 128), F32),
            pltpu.VMEM((NS + 1, 2, NP, 8, 128), F32),
            pltpu.VMEM((NS, G, 128), F32),
            pltpu.VMEM((NS, G, 128), F32),
            pltpu.VMEM((2 * NS, 8, 128), F32),
            pltpu.VMEM((NS, 2, 16, 128), F32),
            pltpu.VMEM((2 * NS, 16, 128), F32),
            pltpu.VMEM((32, 16, 128), F32),
            pltpu.VMEM((8, 16, 128), F32),
            pltpu.VMEM((8, 16, 128), F32),
            pltpu.VMEM((8, 128), F32),
            pltpu.VMEM((16, 128), F32),
            pltpu.VMEM((2, 16, 128), F32),
            dma, dma((NS * PIECES,)), dma, dma((NS * PIECES,)), dma, dma((2 * NS,)),
            dma, dma((2 * NS,)), dma, dma((31,)), dma, dma((8,)), dma, dma((8,)),
        ],
        compiler_params=pltpu.CompilerParams(has_side_effects=True, vmem_limit_bytes=60 * 2**20),
        name="scale_free_fit",
    )(powers, expression)
    return (logdeg, freq, small[:, 0], small[:, 1])


def solution(mesh):
    finer = Mesh(mesh.devices.reshape(4, 2, 2, 2, 8), AXES)
    return jax.shard_map(
        on_device,
        mesh=finer,
        in_specs=(P(AXES, None), P()),
        out_specs=(P(None, AXES), P(), P(), P()),
        check_vma=False,
    )
```

```python
import functools
import math

import jax
import jax.numpy as jnp
from jax import lax
from jax.experimental import pallas as pl
from jax.experimental.pallas import tpu as pltpu
from jax.sharding import Mesh
from jax.sharding import PartitionSpec as P

F32 = jnp.float32
AXES = ("x", "yh", "core", "yl", "z")
NP = 10
BINS = 10
GENES = 32768
S = 1024
G = 128
MESH_ID = pl.DeviceIdType.MESH
OFFSETS = (
    0, 16, 1, 4, 112, 3, 116, 2, 124, 7, 32, 120, 96, 33, 35, 108, 11, 104, 34,
)
HOPS = (
    (0, 0, 0, 2), (0, 1, 1, 5), (0, 1, 4, 1), (0, 0, 5, 4), (0, 1, 2, 3), (0, 1, 5, 4), (0, 1, 0, 2), (0, 0,
    2, 3), (0, 0, 1, 5), (0, 0, 4, 1), (4, 0, 3, 8), (4, 0, 2, 6), (5, 1, 1, 7), (3, 1, 5, 6), (1, 1, 4, 10),
    (2, 0, 0, 7), (4, 1, 3, 8), (4, 1, 5, 12), (1, 0, 4, 10), (3, 0, 1, 9), (5, 1, 2, 9), (10, 1, 0, 13), (8,
    0, 3, 11), (10, 1, 1, 14), (4, 0, 5, 12), (6, 1, 2, 11), (10, 0, 0, 13), (12, 1, 3, 15), (9, 0, 2, 16),
    (10, 0, 1, 14), (8, 0, 5, 15), (13, 1, 0, 18), (9, 1, 2, 16), (11, 0, 5, 17), (15, 1, 3, 17), (13, 0, 0,
    18),
)
ARRIVALS = (
    (1, 1), (2, 0), (3, 1), (4, 0), (5, 1), (1, 0), (2, 1), (3, 0), (4, 1), (5, 0), (8, 0), (6, 0), (6, 1),
    (7, 0), (7, 1), (10, 1), (8, 1), (9, 0), (9, 1), (10, 0), (12, 1), (11, 0), (13, 1), (11, 1), (12, 0),
    (14, 1), (13, 0), (15, 1), (14, 0), (15, 0), (16, 0), (18, 1), (16, 1), (17, 0), (17, 1), (18, 0),
)
PAIRS = (
    (2, 1, 1, 0, 4), (3, 0, 2, 0, 0), (4, 0, 1, 0, 0), (5, 0, 1, 0, 0), (5, 2, 3, 1, 0), (6, 0, 1, 0, 0), (6,
    2, 5, 0, 0), (7, 1, 6, 0, 0), (8, 0, 1, 0, 0), (8, 2, 3, 0, 0), (8, 5, 7, 0, 0), (9, 2, 8, 0, 0), (10, 2,
    4, 0, 0), (10, 5, 6, 0, 0), (10, 8, 9, 0, 0), (11, 2, 7, 0, 0), (12, 9, 10, 0, 3), (13, 4, 6, 0, 0), (13,
    8, 9, 0, 0), (13, 11, 12, 0, 0), (14, 4, 6, 0, 0), (14, 8, 11, 0, 0), (15, 2, 7, 0, 0), (15, 9, 10, 0, 0),
    (15, 13, 14, 0, 0), (16, 2, 7, 1, 0), (16, 13, 15, 0, 0), (17, 0, 1, 0, 0), (17, 2, 10, 0, 2), (17, 12,
    14, 2, 0), (18, 0, 4, 0, 0), (18, 6, 8, 0, 0), (18, 11, 12, 0, 1), (18, 15, 17, 0, 1),
)
STEPS = ((1, 0, 0), (-1, 0, 0), (0, 1, 0), (0, -1, 0), (0, 0, 1), (0, 0, -1))
NS = len(OFFSETS)
PIECES = 2
ROWS = G // PIECES


def offset_of(e):
    return (e & 3, (e >> 2) & 3, e >> 4)


def minus(a, b):
    (ax, ay, az), (bx, by, bz) = offset_of(a), offset_of(b)
    return ((ax - bx) & 3) | (((ay - by) & 3) << 2) | (((az - bz) & 7) << 4)


LEFTS = sorted({0} | {p[1] for p in PAIRS} | {p[2] for p in PAIRS})
LANES = 128


def coded(values, width):
    code = 0
    for v in reversed(values):
        code = code * width + v
    return code


def over_list(values, body):
    for k in range(0, len(values), 6):
        some = values[k : k + 6]

        def step(_, code):
            body(lax.rem(code, 32))
            return lax.div(code, 32)

        lax.fori_loop(0, len(some), step, jnp.int32(coded(some, 32)))


def powers_of(y, lefts, rights, keep, exponents, rows_acc, cols_acc):
    left_sum, left_inv = lefts
    mean = [jnp.broadcast_to(r[2:3, :], (8, 128)) for r in rights]
    inv = [jnp.broadcast_to(r[3:4, :], (8, 128)) * k for r, k in zip(rights, keep, strict=True)]
    cols = [[None] * 2 for _ in range(NP)]
    for band in range(G // 8):
        rows = slice(8 * band, 8 * band + 8)
        m, i = (left_sum[rows, :], left_inv[rows, :])
        logs = [jnp.log2(jnp.abs((y[rows, 128 * h : 128 * h + 128] - m * mean[h]) * i * inv[h])) for h in range(2)]
        for p in range(NP):
            qs = [jnp.exp2(exponents[p] * v) for v in logs]
            cols[p] = [q if old is None else old + q for old, q in zip(cols[p], qs, strict=True)]
            rows_acc[p, rows, :] = rows_acc[p, rows, :] + (qs[0] + qs[1])
    for p in range(NP):
        for h in range(2):
            cols_acc[h, p] = cols_acc[h, p] + cols[p][h]


def lane_row(column):
    return jnp.broadcast_to(column, (128, 128)).T[0:8, :]


def kernel(
    pw, e, logdeg_out, freq_out, small_out,
    X, Y, racc, cacc, LM, LI, ST, PS, RB, DG, ZA, PA, ZB, tile, dsrc, zsrc, fsrc,
    piece_send, piece_recv, pair_send, pair_recv, stat_send, stat_recv,
    part_send, part_recv, plane_send, plane_recv, za_send, za_recv, pa_send, pa_recv, zb_send, zb_recv, acc0, acc1,
):
    px, pyh, c, pyl, pz = [lax.axis_index(a) for a in AXES]
    py = pyh * 2 + pyl
    other = 1 - c

    def at(dx, dy, dz, core):
        y = lax.rem(py + dy + 8, 4)
        return (lax.rem(px + dx + 8, 4), lax.div(y, 2), core, lax.rem(y, 2), lax.rem(pz + dz + 16, 8))

    def remote(src, dst, send, recv, device):
        return pltpu.make_async_remote_copy(
            src_ref=src, dst_ref=dst, send_sem=send, recv_sem=recv, device_id=device, device_id_type=MESH_ID
        )

    partner = at(0, 0, 0, other)
    exponents = [pw[p].astype(F32) for p in range(NP)]

    def piece(slot, q, half):
        return X.at[half, slot, ROWS * q : ROWS * q + ROWS, :]

    def own(q):
        return e.at[ROWS * q : ROWS * q + ROWS, :]

    def hop(i, q, k, j):
        dx, dy, dz = STEPS[k]
        src = own(q) if i == 0 else piece(i, q, c)
        return remote(src, piece(j, q, c), piece_send, piece_recv.at[j * PIECES + q], at(-dx, -dy, -dz, c))

    def to_partner(slot, q):
        src = own(q) if slot == 0 else piece(slot, q, c)
        return remote(src, piece(slot, q, c), pair_send, pair_recv.at[slot * PIECES + q], partner)


    greeted = set()
    for e_ in OFFSETS:
        x, y, z = offset_of(e_)
        for dc in range(2):
            greeted |= {(x, y, z, dc), (-x % 4, -y % 4, -z % 8, dc)}
    for dx, dy, dz in STEPS:
        greeted.add((dx % 4, dy % 4, dz % 8, 0))
    for dc in range(2):
        greeted |= {(dx, dy, 0, dc) for dx in range(4) for dy in range(4)}
    greeted |= {(0, 0, dz, 0) for dz in range(8)}
    greeted = sorted(greeted - {(0, 0, 0, 0)}, key=lambda d: -sum(min(v, n - v) for v, n in zip(d, (4, 4, 8, 2), strict=True)))
    barrier = pltpu.get_barrier_semaphore()
    for dx, dy, dz, dc in greeted:
        pl.semaphore_signal(barrier, inc=1, device_id=at(dx, dy, dz, lax.rem(c + dc, 2)), device_id_type=MESH_ID)

    X[c, 0, :, :] = e[...]
    values = e[...].astype(F32)
    total = jnp.sum(values, axis=1, keepdims=True)
    gene_mean = total * (1.0 / S)
    centred = values - gene_mean
    gene_inv = lax.rsqrt(jnp.sum(centred * centred, axis=1, keepdims=True) * (1.0 / S) + 1e-06)
    row_id = lax.broadcasted_iota(jnp.int32, (8, 128), 0)
    sum_row, inv_row = (lane_row(total), lane_row(gene_inv))
    stats = jnp.where(row_id == 0, sum_row, jnp.where(row_id == 1, inv_row, jnp.where(row_id == 2, sum_row * (1.0 / S), inv_row * (1.0 / S))))
    tile[...] = stats
    ST[pl.ds(c, 1)] = stats[None]

    def stat(slot, half):
        x, y, z = offset_of(OFFSETS[slot])
        return remote(tile, ST.at[2 * slot + c], stat_send, stat_recv.at[2 * slot + c], at(-x, -y, -z, half))

    def stat_in(slot, half):
        x, y, z = offset_of(OFFSETS[slot])
        return remote(tile, ST.at[2 * slot + half], stat_send, stat_recv.at[2 * slot + half], at(-x, -y, -z, half))

    zero = jnp.zeros((NP, 8, 128), F32)

    def clear_rows(s, _):
        for b in range(G // 8):
            racc[s, :, 8 * b : 8 * b + 8, :] = zero
        return 0

    def clear_cols(s, _):
        cacc[s, 0] = zero
        cacc[s, 1] = zero
        return 0

    lax.fori_loop(0, NS, clear_rows, 0)
    lax.fori_loop(0, NS + 1, clear_cols, 0)
    for h in range(2):
        PS[:, h, :, :] = jnp.zeros((NS, 16, 128), F32)

    pl.semaphore_wait(barrier, len(greeted))
    for q in range(PIECES):
        to_partner(0, q).start()
    stat(0, other).start()
    for slot in range(1, NS):
        for half in range(2):
            stat(slot, half).start()
    for i, q, k, j in HOPS:
        if i == 0:
            hop(i, q, k, j).start()

    def ready(slot):
        for q in range(PIECES):
            remote(piece(slot, q, other), piece(slot, q, other), pair_send, pair_recv.at[slot * PIECES + q], partner).wait_recv()
        if slot == 0:
            stat_in(0, other).wait_recv()
        else:
            for half in range(2):
                stat_in(slot, half).wait_recv()
        if slot in LEFTS:
            mine = ST[2 * slot + c]
            LM[slot] = jnp.broadcast_to(mine[0:1, :], (128, 128)).T
            LI[slot] = jnp.broadcast_to(mine[1:2, :], (128, 128)).T

    turns = (lax.rem(lax.div(px, 2), 2), lax.rem(lax.div(py, 2), 2), lax.rem(lax.div(pz, 4), 2))

    def kept(mark):
        turn = jnp.where(mark == 1, turns[0], jnp.where(mark == 2, turns[1], turns[2]))
        h = lax.rem(c + turn, 2)
        return [jnp.where(mark == 0, 1.0, jnp.where(mark == 4, 0.0, jnp.where(h == k, 1.0, 0.0))) for k in range(2)]

    def multiply(b, a0, a1):
        for k in range(2):
            for u in range(2):
                cols = slice(256 * (2 * u + k), 256 * (2 * u + k) + 256)
                rhs = jnp.concatenate([X[0, b, :, cols], X[1, b, :, cols]], axis=0)
                pltpu.matmul_push_rhs(rhs, staging_register=k, mxu_index=u, transpose=True)
        for k in range(2):
            for u, acc in ((0, acc0), (1, acc1)):
                cols = slice(256 * (2 * u + k), 256 * (2 * u + k) + 256)
                lhs = jnp.concatenate([X[c, a0, :, cols], X[c, a1, :, cols]], axis=0)
                pltpu.matmul_acc_lhs(acc, lhs, load_staged_rhs=k)

    def take():
        z = pltpu.matmul_pop(acc0) + pltpu.matmul_pop(acc1)
        Y[0] = z[0:G]
        Y[1] = z[G : 2 * G]

    def use(n, a, b, cols_slot, mark):
        powers_of(Y.at[n], (LM.at[a], LI.at[a]), [ST[2 * b], ST[2 * b + 1]], kept(mark), exponents, racc.at[a], cacc.at[cols_slot])

    def run(pairs, after):
        for k in range(0, len(pairs), 5):
            some = pairs[k : k + 5]
            rest = pairs[k + 5 : k + 6] or [after]
            digits = [coded([p[n] for p in [*some, *rest]], 32) for n in range(3)]
            marks = coded([p[3] * 8 + p[4] for p in some], 64)

            def step(_, codes):
                rights, left0, left1, both = codes
                b, a0, a1, mark = (lax.rem(rights, 32), lax.rem(left0, 32), lax.rem(left1, 32), lax.rem(both, 64))
                rights, left0, left1 = (lax.div(rights, 32), lax.div(left0, 32), lax.div(left1, 32))
                take()
                multiply(lax.rem(rights, 32), lax.rem(left0, 32), lax.rem(left1, 32))
                use(0, a0, b, b, lax.div(mark, 8))
                use(1, a1, b, b, lax.rem(mark, 8))
                return (rights, left0, left1, lax.div(both, 64))

            lax.fori_loop(0, len(some), step, tuple(jnp.int32(v) for v in [*digits, marks]))

    pltpu.matmul_pop(acc0)
    pltpu.matmul_pop(acc1)

    ready(0)
    multiply(0, 0, 0)
    take()

    def own_block(_, x):
        use(0, 0, 0, NS, 0)
        return x

    lax.fori_loop(0, 1, own_block, 0)

    handled = {(0, 0), (0, 1)}
    waiting = list(ARRIVALS)

    def arrive(last):
        while any((last, q) not in handled for q in range(PIECES)):
            slot, q = waiting.pop(0)
            handled.add((slot, q))
            remote(piece(slot, q, c), piece(slot, q, c), piece_send, piece_recv.at[slot * PIECES + q], partner).wait_recv()
            for h in HOPS:
                if h[0] == slot and h[1] == q:
                    hop(*h).start()
            to_partner(slot, q).start()

    known = [0]

    def prepare(last):
        while known[0] < last:
            known[0] += 1
            ready(known[0])

    stages = sorted({p[0] for p in PAIRS})
    arrive(stages[0])
    arrive(stages[1])
    prepare(stages[0])
    first = next(p for p in PAIRS if p[0] == stages[0])
    multiply(*first[0:3])
    for n, b in enumerate(stages):
        arrive(stages[min(n + 2, len(stages) - 1)])
        prepare(stages[min(n + 1, len(stages) - 1)])
        here = [p for p in PAIRS if p[0] == b]
        after = next((p for p in PAIRS if p[0] > b), PAIRS[-1])
        run(here, after)
    pltpu.matmul_pop(acc0)
    pltpu.matmul_pop(acc1)

    def gather_cols(s, _):
        for h in range(2):
            PS[s, h, 0:NP, :] = jnp.sum(cacc[s, h], axis=1)
        return 0

    def gather_rows(s):
        for p in range(NP):
            sums = jnp.sum(racc[s, p].T.reshape(16, 8, 128), axis=0)
            PS[s, c, p : p + 1, :] = PS[s, c, p : p + 1, :] + jnp.sum(sums, axis=0, keepdims=True)

    def part(slot, half):
        x, y, z = offset_of(OFFSETS[slot])
        return remote(PS.at[slot, half], RB.at[2 * slot + c], part_send, part_recv.at[2 * slot + c], at(x, y, z, half))

    def send_parts(slots):
        for slot in slots:
            if slot > 0:
                for half in range(2):
                    part(slot, half).start()

    def far(slot):
        x, y, z = offset_of(OFFSETS[slot])
        return min(x, 4 - x) + min(y, 4 - y) + min(z, 8 - z)

    lax.fori_loop(1, NS, gather_cols, 0)
    send_parts([s for s in range(1, NS) if s not in LEFTS])
    by_distance = sorted(LEFTS, key=lambda s: -far(s))
    for k in range(0, len(by_distance), 6):
        over_list(by_distance[k : k + 6], gather_rows)
        send_parts(by_distance[k : k + 6])
    degree = PS[0, c]
    for slot in range(1, NS):
        for half in range(2):
            remote(PS.at[slot, half], RB.at[2 * slot + half], part_send, part_recv.at[2 * slot + half], partner).wait_recv()
    degree = lax.fori_loop(2, 2 * NS, lambda k, d: d + RB[k], degree)
    dsrc[...] = degree

    me = (px * 4 + py) * 2 + c
    DG[pl.ds(me, 1)] = degree[None]
    plane = [(dx, dy, dc) for dx in range(4) for dy in range(4) for dc in range(2) if (dx, dy, dc) != (0, 0, 0)]

    def plane_hop(n, dx, dy, dc):
        return remote(dsrc, DG.at[me], plane_send, plane_recv.at[n], at(dx, dy, 0, lax.rem(c + dc, 2)))

    def plane_id(dx, dy, dc):
        x, yh, core, yl, _ = at(-dx, -dy, 0, lax.rem(c + dc, 2))
        return (x * 4 + yh * 2 + yl) * 2 + core

    diagonal = lax.broadcasted_iota(jnp.int32, (16, 128), 0) == lax.broadcasted_iota(jnp.int32, (16, 128), 1)

    def to_row(column):
        return jnp.sum(jnp.where(diagonal, column, 0.0), axis=0, keepdims=True)

    def ring(src, buf, send, recv):
        for dz in range(1, 8):
            remote(src, buf.at[pz], send, recv.at[dz], at(0, 0, dz, c)).start()

    def ring_in(src, buf, send, recv):
        for dz in range(1, 8):
            remote(src, buf.at[lax.rem(pz - dz + 8, 8)], send, recv.at[dz], partner).wait_recv()

    mine = to_row(jnp.max(degree, axis=1, keepdims=True))
    zsrc[0] = mine
    ring(zsrc.at[0], ZA, za_send, za_recv)
    for n, h in enumerate(plane):
        plane_hop(n, *h).start()
    logdeg_out[...] = (jnp.log(degree) * (1.0 / math.log(10.0)))[0:NP, :]
    ZA[pl.ds(pz, 1)] = mine[None]
    ring_in(zsrc.at[0], ZA, za_send, za_recv)
    mine = functools.reduce(jnp.maximum, [ZA[k] for k in range(8)])
    zsrc[1] = mine
    for n, (dx, dy, dc) in enumerate(plane):
        remote(zsrc.at[1], PA.at[me], pa_send, pa_recv.at[n], at(dx, dy, 0, lax.rem(c + dc, 2))).start()
    PA[pl.ds(me, 1)] = mine[None]
    for n, h in enumerate(plane):
        remote(dsrc, DG.at[plane_id(*h)], plane_send, plane_recv.at[n], partner).wait_recv()
    for n, h in enumerate(plane):
        remote(zsrc.at[1], PA.at[plane_id(*h)], pa_send, pa_recv.at[n], partner).wait_recv()
    peak_row = functools.reduce(jnp.maximum, [PA[k] for k in range(32)])
    peak = jnp.broadcast_to(jnp.sum(jnp.where(diagonal, peak_row, 0.0), axis=1, keepdims=True), (16, 128))

    def weights(k, sums):
        d = DG[k]
        position = jnp.clip(BINS * d / peak - 0.5, 0.0, BINS - 1.0)
        near = [jnp.maximum(0.0, 1.0 - jnp.abs(position - float(b))) for b in range(BINS)]
        return tuple(s + v for s, v in zip(sums, [*near, d], strict=True))

    sums = lax.fori_loop(0, 32, weights, tuple(jnp.zeros((16, 128), F32) for _ in range(BINS + 1)))
    lanes = lax.broadcasted_iota(jnp.int32, (16, 128), 1)
    found = jnp.zeros((16, 128), F32)
    for b in range(BINS + 1):
        found = jnp.where(lanes == b, jnp.sum(sums[b], axis=1, keepdims=True), found)
    fsrc[...] = found
    ring(fsrc, ZB, zb_send, zb_recv)
    ZB[pl.ds(pz, 1)] = found[None]
    ring_in(fsrc, ZB, zb_send, zb_recv)
    totals = functools.reduce(lambda u, v: u + v, [ZB[k] for k in range(8)])

    log10 = 1.0 / math.log(10.0)
    used = lanes < BINS
    freq = totals * (1.0 / GENES)
    fit_x = jnp.where(used, jnp.log((lanes.astype(F32) + 0.5) * peak / BINS) * log10, 0.0)
    fit_y = jnp.where(used, jnp.log(freq + 1.0 / GENES) * log10, 0.0)
    dev_x = jnp.where(used, fit_x - jnp.sum(fit_x, axis=1, keepdims=True) / BINS, 0.0)
    dev_y = jnp.where(used, fit_y - jnp.sum(fit_y, axis=1, keepdims=True) / BINS, 0.0)
    slope = jnp.sum(dev_x * dev_y, axis=1, keepdims=True) / jnp.sum(dev_x * dev_x, axis=1, keepdims=True)
    mean_log = jnp.log(freq[:, BINS : BINS + 1]) * log10
    freq_out[...] = freq[0:NP, 0:BINS]
    small_out[0:1, :] = to_row(slope)
    small_out[1:2, :] = to_row(mean_log)

    half_x = X.at[0]
    pltpu.make_async_copy(half_x.at[0 : NS - 1], half_x.at[0 : NS - 1], piece_send).wait()
    pltpu.make_async_copy(half_x, half_x, pair_send).wait()
    pltpu.make_async_copy(ST.at[0 : 2 * NS - 1], ST.at[0 : 2 * NS - 1], stat_send).wait()
    pltpu.make_async_copy(RB.at[0 : 2 * NS - 2], RB.at[0 : 2 * NS - 2], part_send).wait()
    pltpu.make_async_copy(DG.at[0:31], DG.at[0:31], plane_send).wait()
    pltpu.make_async_copy(ZA.at[0:7], ZA.at[0:7], za_send).wait()
    pltpu.make_async_copy(PA.at[0:31], PA.at[0:31], pa_send).wait()
    pltpu.make_async_copy(ZB.at[0:7], ZB.at[0:7], zb_send).wait()


def on_device(expression, powers):
    dma = pltpu.SemaphoreType.DMA
    vmem = pl.BlockSpec(memory_space=pltpu.VMEM)
    def body(*refs):
        pl.run_scoped(functools.partial(kernel, *refs), pltpu.ACC(0)((2 * G, 256), F32), pltpu.ACC(1)((2 * G, 256), F32))

    logdeg, freq, small = pl.pallas_call(
        body,
        out_shape=[
            jax.ShapeDtypeStruct((NP, G), F32),
            jax.ShapeDtypeStruct((NP, BINS), F32),
            jax.ShapeDtypeStruct((2, 128), F32),
        ],
        in_specs=[pl.BlockSpec(memory_space=pltpu.SMEM), vmem],
        out_specs=[vmem] * 3,
        scratch_shapes=[
            pltpu.VMEM((2, NS, G, S), jnp.bfloat16),
            pltpu.VMEM((2, G, 2 * G), F32),
            pltpu.VMEM((NS, NP, G, 128), F32),
            pltpu.VMEM((NS + 1, 2, NP, 8, 128), F32),
            pltpu.VMEM((NS, G, 128), F32),
            pltpu.VMEM((NS, G, 128), F32),
            pltpu.VMEM((2 * NS, 8, 128), F32),
            pltpu.VMEM((NS, 2, 16, 128), F32),
            pltpu.VMEM((2 * NS, 16, 128), F32),
            pltpu.VMEM((32, 16, 128), F32),
            pltpu.VMEM((8, 1, 128), F32),
            pltpu.VMEM((32, 1, 128), F32),
            pltpu.VMEM((8, 16, 128), F32),
            pltpu.VMEM((8, 128), F32),
            pltpu.VMEM((16, 128), F32),
            pltpu.VMEM((2, 1, 128), F32),
            pltpu.VMEM((16, 128), F32),
            dma, dma((NS * PIECES,)), dma, dma((NS * PIECES,)), dma, dma((2 * NS,)),
            dma, dma((2 * NS,)), dma, dma((31,)), dma, dma((8,)), dma, dma((31,)), dma, dma((8,)),
        ],
        compiler_params=pltpu.CompilerParams(collective_id=0, has_side_effects=True, vmem_limit_bytes=60 * 2**20),
        name="scale_free_fit",
    )(powers, expression)
    return (logdeg, freq, small[0, 0:NP], small[1, 0:NP])


def solution(mesh):
    finer = Mesh(mesh.devices.reshape(4, 2, 2, 2, 8), AXES)
    return jax.shard_map(
        on_device,
        mesh=finer,
        in_specs=(P(AXES, None), P()),
        out_specs=(P(None, AXES), P(), P(), P()),
        check_vma=False,
    )
```

```python
import functools
import math

import jax
import jax.numpy as jnp
from jax import lax
from jax.experimental import pallas as pl
from jax.experimental.pallas import tpu as pltpu
from jax.sharding import Mesh
from jax.sharding import PartitionSpec as P

F32 = jnp.float32
AXES = ("x", "yh", "core", "yl", "z")
NP = 10
BINS = 10
GENES = 32768
S = 1024
G = 128
MESH_ID = pl.DeviceIdType.MESH
OFFSETS = (
    0, 16, 1, 4, 112, 3, 116, 2, 124, 7, 32, 120, 96, 33, 35, 108, 11, 104, 34,
)
HOPS = (
    (0, 0, 0, 2), (0, 1, 1, 5), (0, 1, 4, 1), (0, 0, 5, 4), (0, 1, 2, 3), (0, 1, 5, 4), (0, 1, 0, 2), (0, 0,
    2, 3), (0, 0, 1, 5), (0, 0, 4, 1), (4, 0, 3, 8), (4, 0, 2, 6), (5, 1, 1, 7), (3, 1, 5, 6), (1, 1, 4, 10),
    (2, 0, 0, 7), (4, 1, 3, 8), (4, 1, 5, 12), (1, 0, 4, 10), (3, 0, 1, 9), (5, 1, 2, 9), (10, 1, 0, 13), (8,
    0, 3, 11), (10, 1, 1, 14), (4, 0, 5, 12), (6, 1, 2, 11), (10, 0, 0, 13), (12, 1, 3, 15), (9, 0, 2, 16),
    (10, 0, 1, 14), (8, 0, 5, 15), (13, 1, 0, 18), (9, 1, 2, 16), (11, 0, 5, 17), (15, 1, 3, 17), (13, 0, 0,
    18),
)
ARRIVALS = (
    (1, 1), (2, 0), (3, 1), (4, 0), (5, 1), (1, 0), (2, 1), (3, 0), (4, 1), (5, 0), (8, 0), (6, 0), (6, 1),
    (7, 0), (7, 1), (10, 1), (8, 1), (9, 0), (9, 1), (10, 0), (12, 1), (11, 0), (13, 1), (11, 1), (12, 0),
    (14, 1), (13, 0), (15, 1), (14, 0), (15, 0), (16, 0), (18, 1), (16, 1), (17, 0), (17, 1), (18, 0),
)
PAIRS = (
    (2, 1, 1, 0, 4), (3, 0, 2, 0, 0), (4, 0, 1, 0, 0), (5, 0, 1, 0, 0), (5, 2, 3, 1, 0), (6, 0, 1, 0, 0), (6,
    2, 5, 0, 0), (7, 1, 6, 0, 0), (8, 0, 1, 0, 0), (8, 2, 3, 0, 0), (8, 5, 7, 0, 0), (9, 2, 8, 0, 0), (10, 2,
    4, 0, 0), (10, 5, 6, 0, 0), (10, 8, 9, 0, 0), (11, 2, 7, 0, 0), (12, 9, 10, 0, 3), (13, 4, 6, 0, 0), (13,
    8, 9, 0, 0), (13, 11, 12, 0, 0), (14, 4, 6, 0, 0), (14, 8, 11, 0, 0), (15, 2, 7, 0, 0), (15, 9, 10, 0, 0),
    (15, 13, 14, 0, 0), (16, 2, 7, 1, 0), (16, 13, 15, 0, 0), (17, 0, 1, 0, 0), (17, 2, 10, 0, 2), (17, 12,
    14, 2, 0), (18, 0, 4, 0, 0), (18, 6, 8, 0, 0), (18, 11, 12, 0, 1), (18, 15, 17, 0, 1),
)
STEPS = ((1, 0, 0), (-1, 0, 0), (0, 1, 0), (0, -1, 0), (0, 0, 1), (0, 0, -1))
NS = len(OFFSETS)
PIECES = 2
ROWS = G // PIECES


def offset_of(e):
    return (e & 3, (e >> 2) & 3, e >> 4)


def minus(a, b):
    (ax, ay, az), (bx, by, bz) = offset_of(a), offset_of(b)
    return ((ax - bx) & 3) | (((ay - by) & 3) << 2) | (((az - bz) & 7) << 4)


FIRST = {j: q for i, q, k, j in reversed(HOPS)}
LEFTS = sorted({0} | {p[1] for p in PAIRS} | {p[2] for p in PAIRS})
LANES = 128


def coded(values, width):
    code = 0
    for v in reversed(values):
        code = code * width + v
    return code


def over_list(values, body):
    for k in range(0, len(values), 6):
        some = values[k : k + 6]

        def step(_, code):
            body(lax.rem(code, 32))
            return lax.div(code, 32)

        lax.fori_loop(0, len(some), step, jnp.int32(coded(some, 32)))


def powers_of(y, lefts, rights, keep, exponents, rows_acc, cols_acc):
    left_sum, left_inv = lefts
    mean = [jnp.broadcast_to(r[2:3, :], (8, 128)) for r in rights]
    inv = [jnp.broadcast_to(r[3:4, :], (8, 128)) * k for r, k in zip(rights, keep, strict=True)]
    cols = [[None] * 2 for _ in range(NP)]
    for band in range(G // 8):
        rows = slice(8 * band, 8 * band + 8)
        m, i = (left_sum[rows, :], left_inv[rows, :])
        logs = [jnp.log2(jnp.abs((y[rows, 128 * h : 128 * h + 128] - m * mean[h]) * i * inv[h])) for h in range(2)]
        for p in range(NP):
            qs = [jnp.exp2(exponents[p] * v) for v in logs]
            cols[p] = [q if old is None else old + q for old, q in zip(cols[p], qs, strict=True)]
            rows_acc[p, rows, :] = rows_acc[p, rows, :] + (qs[0] + qs[1])
    for p in range(NP):
        for h in range(2):
            cols_acc[h, p] = cols_acc[h, p] + cols[p][h]


def lane_row(column):
    return jnp.broadcast_to(column, (128, 128)).T[0:4, :]


def kernel(
    pw, e, logdeg_out, freq_out, small_out,
    X, Y, racc, cacc, LM, LI, ST, PS, RB, DG, ZA, PA, ZB, tile, dsrc, zsrc, fsrc,
    piece_send, piece_recv, pair_send, pair_recv, stat_send, stat_recv,
    part_send, part_recv, plane_send, plane_recv, za_send, za_recv, pa_send, pa_recv, zb_send, zb_recv, acc0, acc1,
):
    px, pyh, c, pyl, pz = [lax.axis_index(a) for a in AXES]
    py = pyh * 2 + pyl
    other = 1 - c

    def at(dx, dy, dz, core):
        y = lax.rem(py + dy + 8, 4)
        return (lax.rem(px + dx + 8, 4), lax.div(y, 2), core, lax.rem(y, 2), lax.rem(pz + dz + 16, 8))

    def remote(src, dst, send, recv, device):
        return pltpu.make_async_remote_copy(
            src_ref=src, dst_ref=dst, send_sem=send, recv_sem=recv, device_id=device, device_id_type=MESH_ID
        )

    partner = at(0, 0, 0, other)
    exponents = [pw[p].astype(F32) for p in range(NP)]

    def piece(slot, q, half):
        return X.at[half, slot, ROWS * q : ROWS * q + ROWS, :]

    def own(q):
        return e.at[ROWS * q : ROWS * q + ROWS, :]

    def hop(i, q, k, j):
        dx, dy, dz = STEPS[k]
        src = own(q) if i == 0 else piece(i, q, c)
        return remote(src, piece(j, q, c), piece_send, piece_recv.at[j * PIECES + q], at(-dx, -dy, -dz, c))

    def to_partner(slot, q):
        src = own(q) if slot == 0 else piece(slot, q, c)
        return remote(src, piece(slot, q, c), pair_send, pair_recv.at[slot * PIECES + q], partner)


    greeted = set()
    for e_ in OFFSETS:
        x, y, z = offset_of(e_)
        for dc in range(2):
            greeted |= {(x, y, z, dc), (-x % 4, -y % 4, -z % 8, dc)}
    for dx, dy, dz in STEPS:
        greeted.add((dx % 4, dy % 4, dz % 8, 0))
    for dc in range(2):
        greeted |= {(dx, dy, 0, dc) for dx in range(4) for dy in range(4)}
    greeted |= {(0, 0, dz, 0) for dz in range(8)}
    greeted = sorted(greeted - {(0, 0, 0, 0)}, key=lambda d: -sum(min(v, n - v) for v, n in zip(d, (4, 4, 8, 2), strict=True)))
    barrier = pltpu.get_barrier_semaphore()
    for dx, dy, dz, dc in greeted:
        pl.semaphore_signal(barrier, inc=1, device_id=at(dx, dy, dz, lax.rem(c + dc, 2)), device_id_type=MESH_ID)

    X[c, 0, :, :] = e[...]
    values = e[...].astype(F32)
    total = jnp.sum(values, axis=1, keepdims=True)
    gene_mean = total * (1.0 / S)
    centred = values - gene_mean
    gene_inv = lax.rsqrt(jnp.sum(centred * centred, axis=1, keepdims=True) * (1.0 / S) + 1e-06)
    row_id = lax.broadcasted_iota(jnp.int32, (4, 128), 0)
    sum_row, inv_row = (lane_row(total), lane_row(gene_inv))
    stats = jnp.where(row_id == 0, sum_row, jnp.where(row_id == 1, inv_row, jnp.where(row_id == 2, sum_row * (1.0 / S), inv_row * (1.0 / S))))
    tile[...] = stats
    ST[pl.ds(c, 1)] = stats[None]

    def stat(slot, half):
        x, y, z = offset_of(OFFSETS[slot])
        return remote(tile, ST.at[2 * slot + c], stat_send, stat_recv.at[2 * slot + c], at(-x, -y, -z, half))

    def stat_in(slot, half):
        x, y, z = offset_of(OFFSETS[slot])
        return remote(tile, ST.at[2 * slot + half], stat_send, stat_recv.at[2 * slot + half], at(-x, -y, -z, half))

    zero = jnp.zeros((NP, 8, 128), F32)

    def clear_rows(s, _):
        for b in range(G // 8):
            racc[s, :, 8 * b : 8 * b + 8, :] = zero
        return 0

    def clear_cols(s, _):
        cacc[s, 0] = zero
        cacc[s, 1] = zero
        return 0

    lax.fori_loop(0, NS, clear_rows, 0)
    lax.fori_loop(0, NS + 1, clear_cols, 0)
    for h in range(2):
        PS[:, h, :, :] = jnp.zeros((NS, 16, 128), F32)

    pl.semaphore_wait(barrier, len(greeted))
    for q in range(PIECES):
        to_partner(0, q).start()
    for i, q, k, j in HOPS:
        if i == 0 and q == FIRST[j]:
            hop(i, q, k, j).start()
    stat(0, other).start()
    for slot in range(1, NS):
        stat(slot, c).start()
    for i, q, k, j in HOPS:
        if i == 0 and q != FIRST[j]:
            hop(i, q, k, j).start()

    def ready(slot):
        for q in range(PIECES):
            remote(piece(slot, q, other), piece(slot, q, other), pair_send, pair_recv.at[slot * PIECES + q], partner).wait_recv()
        stat_in(slot, other).wait_recv()
        if slot in LEFTS:
            mine = ST[2 * slot + c]
            LM[slot] = jnp.broadcast_to(mine[0:1, :], (128, 128)).T
            LI[slot] = jnp.broadcast_to(mine[1:2, :], (128, 128)).T

    turns = (lax.rem(lax.div(px, 2), 2), lax.rem(lax.div(py, 2), 2), lax.rem(lax.div(pz, 4), 2))

    def kept(mark):
        turn = jnp.where(mark == 1, turns[0], jnp.where(mark == 2, turns[1], turns[2]))
        h = lax.rem(c + turn, 2)
        return [jnp.where(mark == 0, 1.0, jnp.where(mark == 4, 0.0, jnp.where(h == k, 1.0, 0.0))) for k in range(2)]

    def multiply(b, a0, a1):
        for k in range(2):
            for u in range(2):
                cols = slice(256 * (2 * u + k), 256 * (2 * u + k) + 256)
                rhs = jnp.concatenate([X[0, b, :, cols], X[1, b, :, cols]], axis=0)
                pltpu.matmul_push_rhs(rhs, staging_register=k, mxu_index=u, transpose=True)
        for k in range(2):
            for u, acc in ((0, acc0), (1, acc1)):
                cols = slice(256 * (2 * u + k), 256 * (2 * u + k) + 256)
                lhs = jnp.concatenate([X[c, a0, :, cols], X[c, a1, :, cols]], axis=0)
                pltpu.matmul_acc_lhs(acc, lhs, load_staged_rhs=k)

    def take():
        z = pltpu.matmul_pop(acc0) + pltpu.matmul_pop(acc1)
        Y[0] = z[0:G]
        Y[1] = z[G : 2 * G]

    def use(n, a, b, cols_slot, mark):
        powers_of(Y.at[n], (LM.at[a], LI.at[a]), [ST[2 * b], ST[2 * b + 1]], kept(mark), exponents, racc.at[a], cacc.at[cols_slot])

    def run(pairs, after):
        for k in range(0, len(pairs), 5):
            some = pairs[k : k + 5]
            rest = pairs[k + 5 : k + 6] or [after]
            digits = [coded([p[n] for p in [*some, *rest]], 32) for n in range(3)]
            marks = coded([p[3] * 8 + p[4] for p in some], 64)

            def step(_, codes):
                rights, left0, left1, both = codes
                b, a0, a1, mark = (lax.rem(rights, 32), lax.rem(left0, 32), lax.rem(left1, 32), lax.rem(both, 64))
                rights, left0, left1 = (lax.div(rights, 32), lax.div(left0, 32), lax.div(left1, 32))
                take()
                multiply(lax.rem(rights, 32), lax.rem(left0, 32), lax.rem(left1, 32))
                use(0, a0, b, b, lax.div(mark, 8))
                use(1, a1, b, b, lax.rem(mark, 8))
                return (rights, left0, left1, lax.div(both, 64))

            lax.fori_loop(0, len(some), step, tuple(jnp.int32(v) for v in [*digits, marks]))

    pltpu.matmul_pop(acc0)
    pltpu.matmul_pop(acc1)

    ready(0)
    multiply(0, 0, 0)
    take()

    def own_block(_, x):
        use(0, 0, 0, NS, 0)
        return x

    lax.fori_loop(0, 1, own_block, 0)

    handled = {(0, 0), (0, 1)}
    waiting = list(ARRIVALS)

    def arrive(last):
        while any((last, q) not in handled for q in range(PIECES)):
            slot, q = waiting.pop(0)
            handled.add((slot, q))
            remote(piece(slot, q, c), piece(slot, q, c), piece_send, piece_recv.at[slot * PIECES + q], partner).wait_recv()
            for h in HOPS:
                if h[0] == slot and h[1] == q:
                    hop(*h).start()
            to_partner(slot, q).start()
            if all((slot, k) in handled for k in range(PIECES)):
                stat_in(slot, c).wait_recv()
                remote(ST.at[2 * slot + c], ST.at[2 * slot + c], stat_send, stat_recv.at[2 * slot + c], partner).start()

    known = [0]

    def prepare(last):
        while known[0] < last:
            known[0] += 1
            ready(known[0])

    stages = sorted({p[0] for p in PAIRS})
    arrive(stages[0])
    arrive(stages[1])
    prepare(stages[0])
    first = next(p for p in PAIRS if p[0] == stages[0])
    multiply(*first[0:3])
    for n, b in enumerate(stages):
        arrive(stages[min(n + 2, len(stages) - 1)])
        prepare(stages[min(n + 1, len(stages) - 1)])
        here = [p for p in PAIRS if p[0] == b]
        after = next((p for p in PAIRS if p[0] > b), PAIRS[-1])
        run(here, after)
    pltpu.matmul_pop(acc0)
    pltpu.matmul_pop(acc1)

    def gather_cols(s, _):
        for h in range(2):
            PS[s, h, 0:NP, :] = jnp.sum(cacc[s, h], axis=1)
        return 0

    def gather_rows(s):
        for p in range(NP):
            sums = jnp.sum(racc[s, p].T.reshape(16, 8, 128), axis=0)
            PS[s, c, p : p + 1, :] = PS[s, c, p : p + 1, :] + jnp.sum(sums, axis=0, keepdims=True)

    def part(slot, half):
        x, y, z = offset_of(OFFSETS[slot])
        return remote(PS.at[slot, half, 0:NP], RB.at[2 * slot + c], part_send, part_recv.at[2 * slot + c], at(x, y, z, half))

    def send_parts(slots):
        for slot in slots:
            if slot > 0:
                for half in range(2):
                    part(slot, half).start()

    def far(slot):
        x, y, z = offset_of(OFFSETS[slot])
        return min(x, 4 - x) + min(y, 4 - y) + min(z, 8 - z)

    lax.fori_loop(1, NS, gather_cols, 0)
    send_parts([s for s in range(1, NS) if s not in LEFTS])
    by_distance = sorted(LEFTS, key=lambda s: -far(s))
    for k in range(0, len(by_distance), 6):
        over_list(by_distance[k : k + 6], gather_rows)
        send_parts(by_distance[k : k + 6])
    degree = PS[0, c, 0:NP, :]
    for slot in range(1, NS):
        for half in range(2):
            remote(PS.at[slot, half, 0:NP], RB.at[2 * slot + half], part_send, part_recv.at[2 * slot + half], partner).wait_recv()
    degree = lax.fori_loop(2, 2 * NS, lambda k, d: d + RB[k], degree)
    dsrc[0:NP, :] = degree

    me = (px * 4 + py) * 2 + c
    DG[pl.ds(me, 1)] = degree[None]
    plane = [(dx, dy, dc) for dx in range(4) for dy in range(4) for dc in range(2) if (dx, dy, dc) != (0, 0, 0)]

    def plane_hop(n, dx, dy, dc):
        return remote(dsrc.at[0:NP], DG.at[me], plane_send, plane_recv.at[n], at(dx, dy, 0, lax.rem(c + dc, 2)))

    def plane_id(dx, dy, dc):
        x, yh, core, yl, _ = at(-dx, -dy, 0, lax.rem(c + dc, 2))
        return (x * 4 + yh * 2 + yl) * 2 + core

    diagonal = lax.broadcasted_iota(jnp.int32, (NP, 128), 0) == lax.broadcasted_iota(jnp.int32, (NP, 128), 1)

    def to_row(column):
        return jnp.sum(jnp.where(diagonal, column, 0.0), axis=0, keepdims=True)

    def ring(src, buf, send, recv):
        for dz in range(1, 8):
            remote(src, buf.at[pz], send, recv.at[dz], at(0, 0, dz, c)).start()

    def ring_in(src, buf, send, recv):
        for dz in range(1, 8):
            remote(src, buf.at[lax.rem(pz - dz + 8, 8)], send, recv.at[dz], partner).wait_recv()

    mine = to_row(jnp.max(degree, axis=1, keepdims=True))
    zsrc[0] = mine
    ring(zsrc.at[0], ZA, za_send, za_recv)
    for n, h in enumerate(plane):
        plane_hop(n, *h).start()
    logdeg_out[...] = jnp.log(degree) * (1.0 / math.log(10.0))
    ZA[pl.ds(pz, 1)] = mine[None]
    ring_in(zsrc.at[0], ZA, za_send, za_recv)
    mine = functools.reduce(jnp.maximum, [ZA[k] for k in range(8)])
    zsrc[1] = mine
    for n, (dx, dy, dc) in enumerate(plane):
        remote(zsrc.at[1], PA.at[me], pa_send, pa_recv.at[n], at(dx, dy, 0, lax.rem(c + dc, 2))).start()
    PA[pl.ds(me, 1)] = mine[None]
    for n, h in enumerate(plane):
        remote(dsrc.at[0:NP], DG.at[plane_id(*h)], plane_send, plane_recv.at[n], partner).wait_recv()
    for n, h in enumerate(plane):
        remote(zsrc.at[1], PA.at[plane_id(*h)], pa_send, pa_recv.at[n], partner).wait_recv()
    peak_row = functools.reduce(jnp.maximum, [PA[k] for k in range(32)])
    peak = jnp.broadcast_to(jnp.sum(jnp.where(diagonal, peak_row, 0.0), axis=1, keepdims=True), (NP, 128))

    def weights(k, sums):
        d = DG[k]
        position = jnp.clip(BINS * d / peak - 0.5, 0.0, BINS - 1.0)
        near = [jnp.maximum(0.0, 1.0 - jnp.abs(position - float(b))) for b in range(BINS)]
        return tuple(s + v for s, v in zip(sums, [*near, d], strict=True))

    sums = lax.fori_loop(0, 32, weights, tuple(jnp.zeros((NP, 128), F32) for _ in range(BINS + 1)))
    lanes = lax.broadcasted_iota(jnp.int32, (NP, 128), 1)
    found = jnp.zeros((NP, 128), F32)
    for b in range(BINS + 1):
        found = jnp.where(lanes == b, jnp.sum(sums[b], axis=1, keepdims=True), found)
    fsrc[...] = found
    ring(fsrc, ZB, zb_send, zb_recv)
    ZB[pl.ds(pz, 1)] = found[None]
    ring_in(fsrc, ZB, zb_send, zb_recv)
    totals = functools.reduce(lambda u, v: u + v, [ZB[k] for k in range(8)])

    log10 = 1.0 / math.log(10.0)
    used = lanes < BINS
    freq = totals * (1.0 / GENES)
    fit_x = jnp.where(used, jnp.log((lanes.astype(F32) + 0.5) * peak / BINS) * log10, 0.0)
    fit_y = jnp.where(used, jnp.log(freq + 1.0 / GENES) * log10, 0.0)
    dev_x = jnp.where(used, fit_x - jnp.sum(fit_x, axis=1, keepdims=True) / BINS, 0.0)
    dev_y = jnp.where(used, fit_y - jnp.sum(fit_y, axis=1, keepdims=True) / BINS, 0.0)
    slope = jnp.sum(dev_x * dev_y, axis=1, keepdims=True) / jnp.sum(dev_x * dev_x, axis=1, keepdims=True)
    mean_log = jnp.log(freq[:, BINS : BINS + 1]) * log10
    freq_out[...] = freq[:, 0:BINS]
    small_out[0:1, :] = to_row(slope)
    small_out[1:2, :] = to_row(mean_log)

    half_x = X.at[0]
    pltpu.make_async_copy(half_x.at[0 : NS - 1], half_x.at[0 : NS - 1], piece_send).wait()
    pltpu.make_async_copy(half_x, half_x, pair_send).wait()
    pltpu.make_async_copy(ST.at[0 : 2 * NS - 1], ST.at[0 : 2 * NS - 1], stat_send).wait()
    pltpu.make_async_copy(RB.at[0 : 2 * NS - 2], RB.at[0 : 2 * NS - 2], part_send).wait()
    pltpu.make_async_copy(DG.at[0:31], DG.at[0:31], plane_send).wait()
    pltpu.make_async_copy(ZA.at[0:7], ZA.at[0:7], za_send).wait()
    pltpu.make_async_copy(PA.at[0:31], PA.at[0:31], pa_send).wait()
    pltpu.make_async_copy(ZB.at[0:7], ZB.at[0:7], zb_send).wait()


def on_device(expression, powers):
    dma = pltpu.SemaphoreType.DMA
    vmem = pl.BlockSpec(memory_space=pltpu.VMEM)
    def body(*refs):
        pl.run_scoped(functools.partial(kernel, *refs), pltpu.ACC(0)((2 * G, 256), F32), pltpu.ACC(1)((2 * G, 256), F32))

    logdeg, freq, small = pl.pallas_call(
        body,
        out_shape=[
            jax.ShapeDtypeStruct((NP, G), F32),
            jax.ShapeDtypeStruct((NP, BINS), F32),
            jax.ShapeDtypeStruct((2, 128), F32),
        ],
        in_specs=[pl.BlockSpec(memory_space=pltpu.SMEM), vmem],
        out_specs=[vmem] * 3,
        scratch_shapes=[
            pltpu.VMEM((2, NS, G, S), jnp.bfloat16),
            pltpu.VMEM((2, G, 2 * G), F32),
            pltpu.VMEM((NS, NP, G, 128), F32),
            pltpu.VMEM((NS + 1, 2, NP, 8, 128), F32),
            pltpu.VMEM((NS, G, 128), F32),
            pltpu.VMEM((NS, G, 128), F32),
            pltpu.VMEM((2 * NS, 4, 128), F32),
            pltpu.VMEM((NS, 2, 16, 128), F32),
            pltpu.VMEM((2 * NS, NP, 128), F32),
            pltpu.VMEM((32, NP, 128), F32),
            pltpu.VMEM((8, 1, 128), F32),
            pltpu.VMEM((32, 1, 128), F32),
            pltpu.VMEM((8, NP, 128), F32),
            pltpu.VMEM((4, 128), F32),
            pltpu.VMEM((NP, 128), F32),
            pltpu.VMEM((2, 1, 128), F32),
            pltpu.VMEM((NP, 128), F32),
            dma, dma((NS * PIECES,)), dma, dma((NS * PIECES,)), dma, dma((2 * NS,)),
            dma, dma((2 * NS,)), dma, dma((31,)), dma, dma((8,)), dma, dma((31,)), dma, dma((8,)),
        ],
        compiler_params=pltpu.CompilerParams(collective_id=0, has_side_effects=True, vmem_limit_bytes=60 * 2**20),
        name="scale_free_fit",
    )(powers, expression)
    return (logdeg, freq, small[0, 0:NP], small[1, 0:NP])


def solution(mesh):
    finer = Mesh(mesh.devices.reshape(4, 2, 2, 2, 8), AXES)
    return jax.shard_map(
        on_device,
        mesh=finer,
        in_specs=(P(AXES, None), P()),
        out_specs=(P(None, AXES), P(), P(), P()),
        check_vma=False,
    )
```

```python
import functools
import math

import jax
import jax.numpy as jnp
from jax import lax
from jax.experimental import pallas as pl
from jax.experimental.pallas import tpu as pltpu
from jax.sharding import Mesh
from jax.sharding import PartitionSpec as P

F32 = jnp.float32
AXES = ("x", "yh", "core", "yl", "z")
NP = 10
BINS = 10
GENES = 32768
S = 1024
G = 128
MESH_ID = pl.DeviceIdType.MESH
OFFSETS = (
    0, 16, 1, 4, 112, 3, 116, 2, 124, 7, 32, 120, 96, 33, 35, 108, 11, 104, 34,
)
HOPS = (
    (0, 0, 0, 2), (0, 1, 1, 5), (0, 1, 4, 1), (0, 0, 5, 4), (0, 1, 2, 3), (0, 1, 5, 4), (0, 1, 0, 2), (0, 0,
    2, 3), (0, 0, 1, 5), (0, 0, 4, 1), (4, 0, 3, 8), (4, 0, 2, 6), (5, 1, 1, 7), (3, 1, 5, 6), (1, 1, 4, 10),
    (2, 0, 0, 7), (4, 1, 3, 8), (4, 1, 5, 12), (1, 0, 4, 10), (3, 0, 1, 9), (5, 1, 2, 9), (10, 1, 0, 13), (8,
    0, 3, 11), (10, 1, 1, 14), (4, 0, 5, 12), (6, 1, 2, 11), (10, 0, 0, 13), (12, 1, 3, 15), (9, 0, 2, 16),
    (10, 0, 1, 14), (8, 0, 5, 15), (13, 1, 0, 18), (9, 1, 2, 16), (11, 0, 5, 17), (15, 1, 3, 17), (13, 0, 0,
    18),
)
ARRIVALS = (
    (1, 1), (2, 0), (3, 1), (4, 0), (5, 1), (1, 0), (2, 1), (3, 0), (4, 1), (5, 0), (8, 0), (6, 0), (6, 1),
    (7, 0), (7, 1), (10, 1), (8, 1), (9, 0), (9, 1), (10, 0), (12, 1), (11, 0), (13, 1), (11, 1), (12, 0),
    (14, 1), (13, 0), (15, 1), (14, 0), (15, 0), (16, 0), (18, 1), (16, 1), (17, 0), (17, 1), (18, 0),
)
PAIRS = (
    (2, 0, 1, 0, 0), (3, 1, 2, 0, 0), (4, 0, 1, 0, 0), (4, 2, 3, 0, 0), (5, 2, 3, 1, 0), (6, 1, 2, 0, 0), (6,
    5, 5, 0, 4), (7, 1, 6, 0, 0), (8, 1, 2, 0, 0), (8, 3, 5, 0, 0), (8, 6, 7, 2, 0), (9, 2, 8, 0, 0), (10, 4,
    6, 0, 0), (10, 8, 9, 0, 0), (11, 1, 2, 0, 0), (11, 7, 10, 0, 0), (12, 5, 7, 0, 0), (12, 9, 10, 0, 3), (13,
    4, 6, 0, 0), (13, 8, 9, 0, 0), (13, 11, 12, 0, 0), (14, 4, 6, 0, 0), (14, 8, 11, 0, 0), (15, 2, 7, 0, 0),
    (15, 10, 12, 0, 0), (15, 13, 14, 0, 0), (16, 2, 7, 1, 0), (16, 12, 15, 0, 0), (17, 2, 7, 0, 0), (17, 10,
    14, 2, 0), (18, 2, 4, 0, 0), (18, 6, 8, 0, 0), (18, 11, 12, 0, 1), (18, 15, 17, 0, 1),
)
STEPS = ((1, 0, 0), (-1, 0, 0), (0, 1, 0), (0, -1, 0), (0, 0, 1), (0, 0, -1))
NS = len(OFFSETS)
PIECES = 2
ROWS = G // PIECES


def offset_of(e):
    return (e & 3, (e >> 2) & 3, e >> 4)


def minus(a, b):
    (ax, ay, az), (bx, by, bz) = offset_of(a), offset_of(b)
    return ((ax - bx) & 3) | (((ay - by) & 3) << 2) | (((az - bz) & 7) << 4)


FIRST = {j: q for i, q, k, j in reversed(HOPS)}
LEFTS = sorted({0} | {p[1] for p in PAIRS} | {p[2] for p in PAIRS})
EARLY = (15,)


def coded(values, width):
    code = 0
    for v in reversed(values):
        code = code * width + v
    return code


def over_list(values, body):
    for k in range(0, len(values), 6):
        some = values[k : k + 6]

        def step(_, code):
            body(lax.rem(code, 32))
            return lax.div(code, 32)

        lax.fori_loop(0, len(some), step, jnp.int32(coded(some, 32)))


def powers_of(y, lefts, rights, keep, exponents, rows_acc, cols_acc):
    left_sum, left_inv = lefts
    mean = [jnp.broadcast_to(r[2:3, :], (8, 128)) for r in rights]
    inv = [jnp.broadcast_to(r[3:4, :], (8, 128)) * k for r, k in zip(rights, keep, strict=True)]
    cols = [[None] * 2 for _ in range(NP)]
    for band in range(G // 8):
        rows = slice(8 * band, 8 * band + 8)
        m, i = (left_sum[rows, :], left_inv[rows, :])
        logs = [jnp.log2(jnp.abs((y[rows, 128 * h : 128 * h + 128] - m * mean[h]) * i * inv[h])) for h in range(2)]
        for p in range(NP):
            qs = [jnp.exp2(exponents[p] * v) for v in logs]
            cols[p] = [q if old is None else old + q for old, q in zip(cols[p], qs, strict=True)]
            rows_acc[p, rows, :] = rows_acc[p, rows, :] + (qs[0] + qs[1])
    for p in range(NP):
        for h in range(2):
            cols_acc[h, p] = cols_acc[h, p] + cols[p][h]


def lane_row(column):
    return jnp.broadcast_to(column, (128, 128)).T[0:4, :]


def kernel(
    pw, e, out,
    X, Y, racc, cacc, LM, LI, ST, PS, RB, DG, ZA, PA, ZB, tile, dsrc, zsrc, fsrc,
    piece_send, piece_recv, pair_send, pair_recv, stat_send, stat_recv,
    part_send, part_recv, plane_send, plane_recv, za_send, za_recv, pa_send, pa_recv, zb_send, zb_recv, acc0, acc1,
):
    px, pyh, c, pyl, pz = [lax.axis_index(a) for a in AXES]
    py = pyh * 2 + pyl
    other = 1 - c

    def at(dx, dy, dz, core):
        y = lax.rem(py + dy + 8, 4)
        return (lax.rem(px + dx + 8, 4), lax.div(y, 2), core, lax.rem(y, 2), lax.rem(pz + dz + 16, 8))

    def remote(src, dst, send, recv, device):
        return pltpu.make_async_remote_copy(
            src_ref=src, dst_ref=dst, send_sem=send, recv_sem=recv, device_id=device, device_id_type=MESH_ID
        )

    partner = at(0, 0, 0, other)
    exponents = [pw[p].astype(F32) for p in range(NP)]

    def piece(slot, q, half):
        return X.at[half, slot, ROWS * q : ROWS * q + ROWS, :]

    def own(q):
        return e.at[ROWS * q : ROWS * q + ROWS, :]

    def hop(i, q, k, j):
        dx, dy, dz = STEPS[k]
        src = own(q) if i == 0 else piece(i, q, c)
        return remote(src, piece(j, q, c), piece_send, piece_recv.at[j * PIECES + q], at(-dx, -dy, -dz, c))

    def to_partner(slot, q):
        src = own(q) if slot == 0 else piece(slot, q, c)
        return remote(src, piece(slot, q, c), pair_send, pair_recv.at[slot * PIECES + q], partner)


    greeted = set()
    for e_ in OFFSETS:
        x, y, z = offset_of(e_)
        for dc in range(2):
            greeted |= {(x, y, z, dc), (-x % 4, -y % 4, -z % 8, dc)}
    for dx, dy, dz in STEPS:
        greeted.add((dx % 4, dy % 4, dz % 8, 0))
    for dc in range(2):
        greeted |= {(dx, dy, 0, dc) for dx in range(4) for dy in range(4)}
    greeted |= {(0, 0, dz, 0) for dz in range(8)}
    greeted = sorted(greeted - {(0, 0, 0, 0)}, key=lambda d: -sum(min(v, n - v) for v, n in zip(d, (4, 4, 8, 2), strict=True)))
    barrier = pltpu.get_barrier_semaphore()
    for dx, dy, dz, dc in greeted:
        pl.semaphore_signal(barrier, inc=1, device_id=at(dx, dy, dz, lax.rem(c + dc, 2)), device_id_type=MESH_ID)

    X[c, 0, :, :] = e[...]
    values = e[...].astype(F32)
    total = jnp.sum(values, axis=1, keepdims=True)
    gene_mean = total * (1.0 / S)
    centred = values - gene_mean
    gene_inv = lax.rsqrt(jnp.sum(centred * centred, axis=1, keepdims=True) * (1.0 / S) + 1e-06)
    row_id = lax.broadcasted_iota(jnp.int32, (4, 128), 0)
    sum_row, inv_row = (lane_row(total), lane_row(gene_inv))
    stats = jnp.where(row_id == 0, sum_row, jnp.where(row_id == 1, inv_row, jnp.where(row_id == 2, sum_row * (1.0 / S), inv_row * (1.0 / S))))
    tile[...] = stats
    ST[pl.ds(c, 1)] = stats[None]

    def stat(slot, half):
        x, y, z = offset_of(OFFSETS[slot])
        return remote(tile, ST.at[2 * slot + c], stat_send, stat_recv.at[2 * slot + c], at(-x, -y, -z, half))

    def stat_in(slot, half):
        x, y, z = offset_of(OFFSETS[slot])
        return remote(tile, ST.at[2 * slot + half], stat_send, stat_recv.at[2 * slot + half], at(-x, -y, -z, half))

    zero = jnp.zeros((NP, 8, 128), F32)

    def clear_rows(s, _):
        for b in range(G // 8):
            racc[s, :, 8 * b : 8 * b + 8, :] = zero
        return 0

    def clear_cols(s, _):
        cacc[s, 0] = zero
        cacc[s, 1] = zero
        return 0

    lax.fori_loop(0, NS, clear_rows, 0)
    lax.fori_loop(0, NS + 1, clear_cols, 0)
    for h in range(2):
        PS[:, h, :, :] = jnp.zeros((NS, 16, 128), F32)

    pl.semaphore_wait(barrier, len(greeted))
    for q in range(PIECES):
        to_partner(0, q).start()
    for i, q, k, j in HOPS:
        if i == 0 and q == FIRST[j]:
            hop(i, q, k, j).start()
    stat(0, other).start()
    for slot in range(1, NS):
        stat(slot, c).start()
    for i, q, k, j in HOPS:
        if i == 0 and q != FIRST[j]:
            hop(i, q, k, j).start()

    def ready(slot):
        for q in range(PIECES):
            remote(piece(slot, q, other), piece(slot, q, other), pair_send, pair_recv.at[slot * PIECES + q], partner).wait_recv()
        stat_in(slot, other).wait_recv()
        if slot in LEFTS:
            mine = ST[2 * slot + c]
            LM[slot] = jnp.broadcast_to(mine[0:1, :], (128, 128)).T
            LI[slot] = jnp.broadcast_to(mine[1:2, :], (128, 128)).T

    turns = (lax.rem(lax.div(px, 2), 2), lax.rem(lax.div(py, 2), 2), lax.rem(lax.div(pz, 4), 2))

    def kept(mark):
        turn = jnp.where(mark == 1, turns[0], jnp.where(mark == 2, turns[1], turns[2]))
        h = lax.rem(c + turn, 2)
        return [jnp.where(mark == 0, 1.0, jnp.where(mark == 4, 0.0, jnp.where(h == k, 1.0, 0.0))) for k in range(2)]

    def multiply(b, a0, a1):
        for k in range(2):
            for u in range(2):
                cols = slice(256 * (2 * u + k), 256 * (2 * u + k) + 256)
                rhs = jnp.concatenate([X[0, b, :, cols], X[1, b, :, cols]], axis=0)
                pltpu.matmul_push_rhs(rhs, staging_register=k, mxu_index=u, transpose=True)
        for k in range(2):
            for u, acc in ((0, acc0), (1, acc1)):
                cols = slice(256 * (2 * u + k), 256 * (2 * u + k) + 256)
                lhs = jnp.concatenate([X[c, a0, :, cols], X[c, a1, :, cols]], axis=0)
                pltpu.matmul_acc_lhs(acc, lhs, load_staged_rhs=k)

    def take():
        z = pltpu.matmul_pop(acc0) + pltpu.matmul_pop(acc1)
        Y[0] = z[0:G]
        Y[1] = z[G : 2 * G]

    def use(n, a, b, cols_slot, mark):
        powers_of(Y.at[n], (LM.at[a], LI.at[a]), [ST[2 * b], ST[2 * b + 1]], kept(mark), exponents, racc.at[a], cacc.at[cols_slot])

    def run(pairs, after):
        for k in range(0, len(pairs), 5):
            some = pairs[k : k + 5]
            rest = pairs[k + 5 : k + 6] or [after]
            digits = [coded([p[n] for p in [*some, *rest]], 32) for n in range(3)]
            marks = coded([p[3] * 8 + p[4] for p in some], 64)

            def step(_, codes):
                rights, left0, left1, both = codes
                b, a0, a1, mark = (lax.rem(rights, 32), lax.rem(left0, 32), lax.rem(left1, 32), lax.rem(both, 64))
                rights, left0, left1 = (lax.div(rights, 32), lax.div(left0, 32), lax.div(left1, 32))
                take()
                multiply(lax.rem(rights, 32), lax.rem(left0, 32), lax.rem(left1, 32))
                use(0, a0, b, b, lax.div(mark, 8))
                use(1, a1, b, b, lax.rem(mark, 8))
                return (rights, left0, left1, lax.div(both, 64))

            lax.fori_loop(0, len(some), step, tuple(jnp.int32(v) for v in [*digits, marks]))

    pltpu.matmul_pop(acc0)
    pltpu.matmul_pop(acc1)

    ready(0)
    multiply(0, 0, 0)
    take()

    def own_block(_, x):
        use(0, 0, 0, NS, 0)
        return x

    lax.fori_loop(0, 1, own_block, 0)

    handled = {(0, 0), (0, 1)}
    waiting = list(ARRIVALS)

    def arrive(last):
        while any((last, q) not in handled for q in range(PIECES)):
            slot, q = waiting.pop(0)
            handled.add((slot, q))
            remote(piece(slot, q, c), piece(slot, q, c), piece_send, piece_recv.at[slot * PIECES + q], partner).wait_recv()
            for h in HOPS:
                if h[0] == slot and h[1] == q:
                    hop(*h).start()
            to_partner(slot, q).start()
            if all((slot, k) in handled for k in range(PIECES)):
                stat_in(slot, c).wait_recv()
                remote(ST.at[2 * slot + c], ST.at[2 * slot + c], stat_send, stat_recv.at[2 * slot + c], partner).start()

    known = [0]

    def prepare(last):
        while known[0] < last:
            known[0] += 1
            ready(known[0])

    def gather_cols(s, _):
        for h in range(2):
            PS[s, h, 0:NP, :] = PS[s, h, 0:NP, :] + jnp.sum(cacc[s, h], axis=1)
        return 0

    def gather_rows(s):
        for p in range(NP):
            sums = jnp.sum(racc[s, p].T.reshape(16, 8, 128), axis=0)
            PS[s, c, p : p + 1, :] = PS[s, c, p : p + 1, :] + jnp.sum(sums, axis=0, keepdims=True)

    stages = sorted({p[0] for p in PAIRS})
    last_use = {a: max(p[0] for p in PAIRS if a in p[1:3]) for a in LEFTS}
    gathered = []
    arrive(stages[0])
    arrive(stages[1])
    prepare(stages[0])
    first = next(p for p in PAIRS if p[0] == stages[0])
    multiply(*first[0:3])
    for n, b in enumerate(stages):
        if stages[min(n + 2, len(stages) - 1)] in EARLY:
            done = [a for a in LEFTS if last_use[a] < b and a not in gathered]
            over_list(done, gather_rows)
            gathered.extend(done)
        arrive(stages[min(n + 2, len(stages) - 1)])
        prepare(stages[min(n + 1, len(stages) - 1)])
        here = [p for p in PAIRS if p[0] == b]
        after = next((p for p in PAIRS if p[0] > b), PAIRS[-1])
        run(here, after)
    pltpu.matmul_pop(acc0)
    pltpu.matmul_pop(acc1)

    def part(slot, half):
        x, y, z = offset_of(OFFSETS[slot])
        return remote(PS.at[slot, half, 0:NP], RB.at[2 * slot + c], part_send, part_recv.at[2 * slot + c], at(x, y, z, half))

    def send_parts(slots):
        for slot in slots:
            if slot > 0:
                for half in range(2):
                    part(slot, half).start()

    def far(slot):
        x, y, z = offset_of(OFFSETS[slot])
        return min(x, 4 - x) + min(y, 4 - y) + min(z, 8 - z)

    lax.fori_loop(1, NS, gather_cols, 0)
    send_parts([s for s in range(1, NS) if s not in LEFTS or s in gathered])
    by_distance = sorted((s for s in LEFTS if s not in gathered), key=lambda s: -far(s))
    for k in range(0, len(by_distance), 6):
        over_list(by_distance[k : k + 6], gather_rows)
        send_parts(by_distance[k : k + 6])
    degree = PS[0, c, 0:NP, :]
    for slot in range(1, NS):
        for half in range(2):
            remote(PS.at[slot, half, 0:NP], RB.at[2 * slot + half], part_send, part_recv.at[2 * slot + half], partner).wait_recv()
    degree = lax.fori_loop(2, 2 * NS, lambda k, d: d + RB[k], degree)
    dsrc[0:NP, :] = degree

    me = (px * 4 + py) * 2 + c
    DG[pl.ds(me, 1)] = degree[None]
    plane = [(dx, dy, dc) for dx in range(4) for dy in range(4) for dc in range(2) if (dx, dy, dc) != (0, 0, 0)]

    def plane_hop(n, dx, dy, dc):
        return remote(dsrc.at[0:NP], DG.at[me], plane_send, plane_recv.at[n], at(dx, dy, 0, lax.rem(c + dc, 2)))

    def plane_id(dx, dy, dc):
        x, yh, core, yl, _ = at(-dx, -dy, 0, lax.rem(c + dc, 2))
        return (x * 4 + yh * 2 + yl) * 2 + core

    diagonal = lax.broadcasted_iota(jnp.int32, (NP, 128), 0) == lax.broadcasted_iota(jnp.int32, (NP, 128), 1)

    def to_row(column):
        return jnp.sum(jnp.where(diagonal, column, 0.0), axis=0, keepdims=True)

    def ring(src, buf, send, recv):
        for dz in range(1, 8):
            remote(src, buf.at[pz], send, recv.at[dz], at(0, 0, dz, c)).start()

    def ring_in(src, buf, send, recv):
        for dz in range(1, 8):
            remote(src, buf.at[lax.rem(pz - dz + 8, 8)], send, recv.at[dz], partner).wait_recv()

    mine = to_row(jnp.max(degree, axis=1, keepdims=True))
    zsrc[0] = mine
    ring(zsrc.at[0], ZA, za_send, za_recv)
    for n, h in enumerate(plane):
        plane_hop(n, *h).start()
    out[0:NP, :] = jnp.log(degree) * (1.0 / math.log(10.0))
    ZA[pl.ds(pz, 1)] = mine[None]
    ring_in(zsrc.at[0], ZA, za_send, za_recv)
    mine = functools.reduce(jnp.maximum, [ZA[k] for k in range(8)])
    zsrc[1] = mine
    for n, (dx, dy, dc) in enumerate(plane):
        remote(zsrc.at[1], PA.at[me], pa_send, pa_recv.at[n], at(dx, dy, 0, lax.rem(c + dc, 2))).start()
    PA[pl.ds(me, 1)] = mine[None]
    for n, h in enumerate(plane):
        remote(dsrc.at[0:NP], DG.at[plane_id(*h)], plane_send, plane_recv.at[n], partner).wait_recv()
    for n, h in enumerate(plane):
        remote(zsrc.at[1], PA.at[plane_id(*h)], pa_send, pa_recv.at[n], partner).wait_recv()
    peak_row = functools.reduce(jnp.maximum, [PA[k] for k in range(32)])
    peak = jnp.broadcast_to(jnp.sum(jnp.where(diagonal, peak_row, 0.0), axis=1, keepdims=True), (NP, 128))

    def weights(k, sums):
        d = DG[k]
        position = jnp.clip(BINS * d / peak - 0.5, 0.0, BINS - 1.0)
        near = [jnp.maximum(0.0, 1.0 - jnp.abs(position - float(b))) for b in range(BINS)]
        return tuple(s + v for s, v in zip(sums, [*near, d], strict=True))

    sums = lax.fori_loop(0, 32, weights, tuple(jnp.zeros((NP, 128), F32) for _ in range(BINS + 1)))
    lanes = lax.broadcasted_iota(jnp.int32, (NP, 128), 1)
    found = jnp.zeros((NP, 128), F32)
    for b in range(BINS + 1):
        found = jnp.where(lanes == b, jnp.sum(sums[b], axis=1, keepdims=True), found)
    fsrc[...] = found
    ring(fsrc, ZB, zb_send, zb_recv)
    ZB[pl.ds(pz, 1)] = found[None]
    ring_in(fsrc, ZB, zb_send, zb_recv)
    totals = functools.reduce(lambda u, v: u + v, [ZB[k] for k in range(8)])

    log10 = 1.0 / math.log(10.0)
    used = lanes < BINS
    freq = totals * (1.0 / GENES)
    fit_x = jnp.where(used, jnp.log((lanes.astype(F32) + 0.5) * peak / BINS) * log10, 0.0)
    fit_y = jnp.where(used, jnp.log(freq + 1.0 / GENES) * log10, 0.0)
    dev_x = jnp.where(used, fit_x - jnp.sum(fit_x, axis=1, keepdims=True) / BINS, 0.0)
    dev_y = jnp.where(used, fit_y - jnp.sum(fit_y, axis=1, keepdims=True) / BINS, 0.0)
    slope = jnp.sum(dev_x * dev_y, axis=1, keepdims=True) / jnp.sum(dev_x * dev_x, axis=1, keepdims=True)
    mean_log = jnp.log(freq[:, BINS : BINS + 1]) * log10
    out[16 : 16 + NP, :] = freq
    out[32:33, :] = to_row(slope)
    out[33:34, :] = to_row(mean_log)

    half_x = X.at[0]
    pltpu.make_async_copy(half_x.at[0 : NS - 1], half_x.at[0 : NS - 1], piece_send).wait()
    pltpu.make_async_copy(half_x, half_x, pair_send).wait()
    pltpu.make_async_copy(ST.at[0 : 2 * NS - 1], ST.at[0 : 2 * NS - 1], stat_send).wait()
    pltpu.make_async_copy(RB.at[0 : 2 * NS - 2], RB.at[0 : 2 * NS - 2], part_send).wait()
    pltpu.make_async_copy(DG.at[0:31], DG.at[0:31], plane_send).wait()
    pltpu.make_async_copy(ZA.at[0:7], ZA.at[0:7], za_send).wait()
    pltpu.make_async_copy(PA.at[0:31], PA.at[0:31], pa_send).wait()
    pltpu.make_async_copy(ZB.at[0:7], ZB.at[0:7], zb_send).wait()


def on_device(expression, powers):
    dma = pltpu.SemaphoreType.DMA
    vmem = pl.BlockSpec(memory_space=pltpu.VMEM)
    def body(*refs):
        pl.run_scoped(functools.partial(kernel, *refs), pltpu.ACC(0)((2 * G, 256), F32), pltpu.ACC(1)((2 * G, 256), F32))

    packed = pl.pallas_call(
        body,
        out_shape=jax.ShapeDtypeStruct((40, 128), F32),
        in_specs=[pl.BlockSpec(memory_space=pltpu.SMEM), vmem],
        out_specs=vmem,
        scratch_shapes=[
            pltpu.VMEM((2, NS, G, S), jnp.bfloat16),
            pltpu.VMEM((2, G, 2 * G), F32),
            pltpu.VMEM((NS, NP, G, 128), F32),
            pltpu.VMEM((NS + 1, 2, NP, 8, 128), F32),
            pltpu.VMEM((NS, G, 128), F32),
            pltpu.VMEM((NS, G, 128), F32),
            pltpu.VMEM((2 * NS, 4, 128), F32),
            pltpu.VMEM((NS, 2, 16, 128), F32),
            pltpu.VMEM((2 * NS, NP, 128), F32),
            pltpu.VMEM((32, NP, 128), F32),
            pltpu.VMEM((8, 1, 128), F32),
            pltpu.VMEM((32, 1, 128), F32),
            pltpu.VMEM((8, NP, 128), F32),
            pltpu.VMEM((4, 128), F32),
            pltpu.VMEM((NP, 128), F32),
            pltpu.VMEM((2, 1, 128), F32),
            pltpu.VMEM((NP, 128), F32),
            dma, dma((NS * PIECES,)), dma, dma((NS * PIECES,)), dma, dma((2 * NS,)),
            dma, dma((2 * NS,)), dma, dma((31,)), dma, dma((8,)), dma, dma((31,)), dma, dma((8,)),
        ],
        compiler_params=pltpu.CompilerParams(collective_id=0, has_side_effects=True, vmem_limit_bytes=60 * 2**20),
        name="scale_free_fit",
    )(powers, expression)
    return (packed[0:NP], packed[16 : 16 + NP, 0:BINS], packed[32, 0:NP], packed[33, 0:NP])


def solution(mesh):
    finer = Mesh(mesh.devices.reshape(4, 2, 2, 2, 8), AXES)
    return jax.shard_map(
        on_device,
        mesh=finer,
        in_specs=(P(AXES, None), P()),
        out_specs=(P(None, AXES), P(), P(), P()),
        check_vma=False,
    )
```
